128 devices in a mesh: pipe: 2 (over x_lo), tensor: 4 (over x_hi, core), dp: 16 (over z, y).
Axes of the slice: x: 4 (x_hi: 2, x_lo: 2; x = x_hi * 2 + x_lo), y: 4, z: 4, core: 2. Of those that a mesh axis runs over, the one named last changes fastest.
Arguments:
- inputs: bfloat16 [2, 2048, 16384], P(None, 'dp', 'tensor'), may hold values from -6 to 6
- w_in: bfloat16 [2, 16384, 1024], P('pipe', ('tensor', 'dp')), may hold values from -0.046875 to 0.046875
- w_out: bfloat16 [2, 1024, 16384], P('pipe', None, ('tensor', 'dp')), may hold values from -0.1875 to 0.1875
- cotangent: bfloat16 [2, 2048, 16384], P(None, 'dp', 'tensor'), may hold values from -6 to 6
Outputs:
- update_in: float32 [2, 16384, 1024], P('pipe', ('tensor', 'dp'))
- update_out: float32 [2, 1024, 16384], P('pipe', None, ('tensor', 'dp'))
- grad_norm: float32 [], replicated
The draws below stay inside these ranges and needn't reach their ends.
All inputs are finite; a program needn't handle non-finite values.
Results may differ from the reference program's by a relative error of at most 0.008.
Values may be sent and summed in bfloat16 or wider, within the bound.
A program may use at most 192 MiB of HBM per device.

```python
import jax
import jax.numpy as jnp
from jax import lax

D = 16384
H = 1024
MB = 2
TOK = 128
SECTIONS = 2
BATCH = 2048
CLIP_NORM = 16384


def steps_of(key, dims, cuts, low, high):
    def one(dim, shards_of):
        draws = jax.random.uniform(jax.random.fold_in(jax.random.fold_in(key, 6), dim), (shards_of,), jnp.float32, low / len(cuts), high / len(cuts))
        return jnp.repeat(jnp.exp(draws), dims[dim] // shards_of).reshape((-1,) + (1,) * (len(dims) - dim - 1))

    gain = one(*cuts[0])
    for cut in cuts[1:]:
        gain = gain * one(*cut)
    return gain


def gaussian(key, extent, scale, most, split=(), dtype=jnp.bfloat16):
    gain = steps_of(key, extent, split, -0.22, 0.18) if split else 1.0
    values = jax.random.normal(key, extent, jnp.float32) * scale * gain
    return jnp.minimum(jnp.maximum(values, -most), most).astype(dtype)


def setup_inputs(seed: int = 0) -> dict:
    keys = jax.random.split(jax.random.key(seed), 5)
    return {
        "inputs": gaussian(keys[0], (MB, BATCH, D), 1.0, 6.0, ((1, 16), (2, 4))),
        "w_in": gaussian(keys[1], (SECTIONS, D, H), D ** -0.5, 0.046875, ((0, 2), (1, 64))),
        "w_out": gaussian(keys[2], (SECTIONS, H, D), H ** -0.5, 0.1875, ((0, 2), (2, 64))),
        "cotangent": gaussian(keys[3], (MB, BATCH, D), 1.0, 6.0, ((1, 16), (2, 4))),
    }


def silu_round(preact):
    return jax.nn.silu(preact).astype(jnp.bfloat16)

def slope_round(upward, preact):
    sigmoid_value = jax.nn.sigmoid(preact)
    return (upward * sigmoid_value * (1.0 + preact * (1.0 - sigmoid_value))).astype(jnp.bfloat16)

def kahan_add(running, carried, grad_term):
    corrected = grad_term - carried.astype(jnp.float32)
    summed = (running.astype(jnp.float32) + corrected).astype(jnp.bfloat16)
    carried = (summed.astype(jnp.float32) - running.astype(jnp.float32) - corrected).astype(jnp.bfloat16)
    return (summed, carried)

def reference(inputs, w_in, w_out, cotangent):
    replicas = BATCH // TOK
    stored_x = []
    stored_pre = []
    stored_act = []
    for micro_index in range(MB):
        current = inputs[micro_index]
        list_x, list_pre, list_act = ([], [], [])
        for layer in range(SECTIONS):
            preact = jnp.dot(current, w_in[layer], preferred_element_type=jnp.float32)
            activation = silu_round(preact)
            list_x.append(current)
            list_pre.append(preact)
            list_act.append(activation)
            current = (current.astype(jnp.float32) + jnp.dot(activation, w_out[layer], preferred_element_type=jnp.float32)).astype(jnp.bfloat16)
        stored_x.append(list_x)
        stored_pre.append(list_pre)
        stored_act.append(list_act)
    errors = [cotangent[micro_index] for micro_index in range(MB)]
    totals_in = [None] * SECTIONS
    totals_out = [None] * SECTIONS
    for layer in reversed(range(SECTIONS)):
        sum_in = jnp.zeros((replicas, D, H), jnp.bfloat16)
        err_in = jnp.zeros((replicas, D, H), jnp.bfloat16)
        sum_out = jnp.zeros((replicas, H, D), jnp.bfloat16)
        err_out = jnp.zeros((replicas, H, D), jnp.bfloat16)
        for micro_index in range(MB):
            upper = errors[micro_index]
            upward = jnp.dot(upper, w_out[layer].T, preferred_element_type=jnp.float32)
            slope = slope_round(upward, stored_pre[micro_index][layer])
            x_groups = stored_x[micro_index][layer].reshape(replicas, TOK, D).astype(jnp.float32)
            slope_groups = slope.reshape(replicas, TOK, H).astype(jnp.float32)
            act_groups = stored_act[micro_index][layer].reshape(replicas, TOK, H).astype(jnp.float32)
            err_groups = upper.reshape(replicas, TOK, D).astype(jnp.float32)
            grad_in = jnp.einsum('gtc,gth->gch', x_groups, slope_groups)
            grad_out = jnp.einsum('gth,gtc->ghc', act_groups, err_groups)
            sum_in, err_in = kahan_add(sum_in, err_in, grad_in)
            sum_out, err_out = kahan_add(sum_out, err_out, grad_out)
            errors[micro_index] = (upper.astype(jnp.float32) + jnp.dot(slope, w_in[layer].T, preferred_element_type=jnp.float32)).astype(jnp.bfloat16)
        totals_in[layer] = lax.optimization_barrier(jnp.sum(sum_in.astype(jnp.float32) - err_in.astype(jnp.float32), axis=0))
        totals_out[layer] = lax.optimization_barrier(jnp.sum(sum_out.astype(jnp.float32) - err_out.astype(jnp.float32), axis=0))
    total_in = jnp.stack(totals_in)
    total_out = jnp.stack(totals_out)
    grad_norm = jnp.sqrt(jnp.sum(total_in * total_in) + jnp.sum(total_out * total_out))
    factor = jnp.minimum(1.0, CLIP_NORM / grad_norm)
    return (total_in * factor, total_out * factor, grad_norm)
```

```python
import jax
import jax.numpy as jnp
from jax import lax
from jax.experimental import pallas as pl
from jax.experimental.pallas import tpu as pltpu
from jax.sharding import Mesh
from jax.sharding import PartitionSpec as P

CLIP_NORM = 16384.0
AXES = ("pipe", "xhi", "core", "z", "y")
TENSOR = ("xhi", "core")
DP = ("z", "y")
PIPE_TENSOR_DP = ("pipe", "xhi", "core", "z", "y")
TENSOR_DP = ("xhi", "core", "z", "y")
MESH = pl.DeviceIdType.MESH
BF = jnp.bfloat16
F32 = jnp.float32

RING = 4
REP = RING * RING
GROUP = 8
NT = (((1,), (1,)), ((), ()))
TN = (((0,), (0,)), ((), ()))


def kernel(
    x_hbm, win_hbm, wot_hbm, cot_hbm,
    upd_in, upd_out, norm_out,
    x0, cot, x1, err1, w, g, act, slope, part, xrecv, r1a, r1b, r2a, r2b,
    fin, pex, prx, nsum, nz, ny, nx, pre_keep,
    lsem, ssem, rsem,
):
    micro, tok, half_d = x0.shape
    rows = micro * tok
    hid = w.shape[-1]
    sub = w.shape[3]
    hl = hid // 2
    chunk = rows // GROUP
    pipe = lax.axis_index("pipe")
    xhi = lax.axis_index("xhi")
    core = lax.axis_index("core")
    z = lax.axis_index("z")
    y = lax.axis_index("y")
    other = 1 - pipe
    c_me = pipe * 4 + xhi * 2 + core

    def turn(v, d):
        return lax.rem(v + d, RING)

    started = []
    count = [0]
    lcount = [0]

    def remote(src, dst, dev):
        i = count[0]
        count[0] += 1
        copy = pltpu.make_async_remote_copy(
            src_ref=src, dst_ref=dst, send_sem=ssem.at[i], recv_sem=rsem.at[i],
            device_id=dev, device_id_type=MESH,
        )
        copy.start()
        started.append(copy)
        return copy

    def local(src, dst):
        i = lcount[0]
        lcount[0] += 1
        copy = pltpu.make_async_copy(src, dst, lsem.at[i])
        copy.start()
        return copy

    def wait_all(copies):
        for copy in copies:
            copy.wait_recv()

    xpeers = []
    for code in range(1, GROUP):
        a, b, c = code // 4, (code // 2) % 2, code % 2
        p_ = other if a else pipe
        h_ = 1 - xhi if b else xhi
        c_ = 1 - core if c else core
        xpeers.append((code, {"pipe": p_, "xhi": h_, "core": c_}, p_ * 4 + h_ * 2 + c_))

    own_w = [
        local(win_hbm.at[pl.ds(pl.multiple_of(pipe * sub, sub), sub), :], w.at[2 * pipe, z, y]),
        local(wot_hbm.at[pl.ds(pl.multiple_of(pipe * sub, sub), sub), :], w.at[2 * pipe + 1, z, y]),
    ]
    loads = {}
    for name, src, dst in (("x", x_hbm, x0), ("cot", cot_hbm, cot)):
        loads[name] = []
        for r in range(REP):
            off = pl.multiple_of(r * 2 * sub + pipe * sub, sub)
            loads[name].append(
                local(src.at[:, :, pl.ds(off, sub)], dst.at[:, :, pl.ds(r * sub, sub)])
            )

    barrier = pltpu.get_barrier_semaphore()
    peers = [dev for _, dev, _ in xpeers]
    for d in range(1, RING):
        peers.append({"z": turn(z, d)})
        peers.append({"y": turn(y, d)})
    for dev in peers:
        pl.semaphore_signal(barrier, inc=1, device_id=dev, device_id_type=MESH)
    pl.semaphore_wait(barrier, len(peers))

    pair = {"pipe": other}
    give = []
    for kind, src in ((0, win_hbm), (1, wot_hbm)):
        give.append(
            remote(
                src.at[pl.ds(pl.multiple_of(other * sub, sub), sub), :],
                w.at[2 * pipe + kind, z, y],
                pair,
            )
        )

    A, B = pl.ds(0, hl), pl.ds(hl, hl)
    up_z, dn_z = {"z": turn(z, 1)}, {"z": turn(z, 3)}
    up_y, dn_y = {"y": turn(y, 1)}, {"y": turn(y, 3)}
    hs = sub // 2

    def same(ref, dev):
        return remote(ref, ref, dev)

    def g1a(k):
        a, b = w.at[k, z, y, :, A], w.at[k, z, y, :, B]
        return [same(a, up_y), same(a, dn_y), same(b, up_z), same(b, dn_z)]

    def g1b(k):
        return [
            same(w.at[k, z, turn(y, 3), pl.ds(0, hs), A], up_y),
            same(w.at[k, z, turn(y, 1), pl.ds(hs, hs), A], dn_y),
            same(w.at[k, turn(z, 3), y, pl.ds(0, hs), B], up_z),
            same(w.at[k, turn(z, 1), y, pl.ds(hs, hs), B], dn_z),
        ]

    def g2a(k):
        a, b = w.at[k, z, :, :, A], w.at[k, :, y, :, B]
        return [same(a, up_z), same(a, dn_z), same(b, up_y), same(b, dn_y)]

    def g2b(k):
        return [
            same(w.at[k, turn(z, 3), pl.ds(0, 2), :, A], up_z),
            same(w.at[k, turn(z, 1), pl.ds(2, 2), :, A], dn_z),
            same(w.at[k, pl.ds(0, 2), turn(y, 3), :, B], up_y),
            same(w.at[k, pl.ds(2, 2), turn(y, 1), :, B], dn_y),
        ]

    tile = 256

    def project(src, k, ph):
        @pl.loop(0, hid // tile)
        def _(n):
            cols = pl.ds(pl.multiple_of(n * tile, tile), tile)
            left = src[...].reshape(rows, half_d)
            right = w[k, :, :, :, cols].reshape(half_d, tile)
            part[ph, :, cols] = jnp.dot(left, right, preferred_element_type=F32).astype(BF)

    def widen(base, units, k, out):
        def wide(base_ref, units_ref, out_ref):
            for zz in range(RING):
                @pl.loop(0, 2)
                def _(q):
                    cols = pl.ds(pl.multiple_of(zz * 4 * sub + q * 2 * sub, tile), 2 * sub)
                    right = w[k, zz, pl.ds(q * 2, 2), :, :].reshape(2 * sub, hid)
                    add = lax.dot_general(units_ref, right, NT, preferred_element_type=F32)
                    old = base_ref[:, :, cols].reshape(rows, 2 * sub).astype(F32)
                    out_ref[:, :, cols] = (old + add).astype(BF).reshape(micro, tok, 2 * sub)

        wide(base, units[...], out)

    def weight_grad(left_ref, right, k):
        for zz in range(RING):
            @pl.loop(0, 2)
            def _(q):
                cols = pl.ds(pl.multiple_of(zz * 4 * sub + q * 2 * sub, tile), 2 * sub)
                left = left_ref[:, :, cols].reshape(rows, 2 * sub)
                got = lax.dot_general(left, right[...], TN, preferred_element_type=F32)
                g[k, zz, pl.ds(q * 2, 2), :, :] = got.astype(BF).reshape(2, sub, hid)

    def scatter_units(ph):
        copies = []
        for code, dev, c in xpeers:
            at = pl.ds(pl.multiple_of(c * chunk, chunk), chunk)
            copies.append(remote(part.at[ph, at, :], xrecv.at[ph, code], dev))
        return copies

    mine = pl.ds(pl.multiple_of(c_me * chunk, chunk), chunk)

    def units_sum(ph):
        total = part[ph, mine, :].astype(F32)
        for code in range(1, GROUP):
            total = total + xrecv[ph, code].astype(F32)
        return total

    def spread_units(ref, value):
        ref[mine, :] = value
        return [remote(ref.at[mine, :], ref.at[mine, :], dev) for _, dev, _ in xpeers]

    def slope_of(up, pre):
        s = jax.nn.sigmoid(pre)
        return (up * s * (1.0 + pre * (1.0 - s))).astype(BF)

    def s1a(k):
        z2, y2 = turn(z, 2), turn(y, 2)
        return [
            remote(g.at[k, z2, pl.ds(0, 2), :, A], r1a.at[k, 0, 0], up_z),
            remote(g.at[k, z2, pl.ds(2, 2), :, A], r1a.at[k, 0, 1], dn_z),
            remote(g.at[k, pl.ds(0, 2), y2, :, B], r1a.at[k, 1, 0], up_y),
            remote(g.at[k, pl.ds(2, 2), y2, :, B], r1a.at[k, 1, 1], dn_y),
        ]

    def s1b(k):
        zu, zd, yu, yd = turn(z, 1), turn(z, 3), turn(y, 1), turn(y, 3)

        @pl.loop(0, 2)
        def _(q):
            g[k, zu, q, :, A] = (g[k, zu, q, :, A].astype(F32) + r1a[k, 0, 0, q].astype(F32)).astype(BF)
            g[k, zd, q + 2, :, A] = (
                g[k, zd, q + 2, :, A].astype(F32) + r1a[k, 0, 1, q].astype(F32)
            ).astype(BF)
            g[k, q, yu, :, B] = (g[k, q, yu, :, B].astype(F32) + r1a[k, 1, 0, q].astype(F32)).astype(BF)
            g[k, q + 2, yd, :, B] = (
                g[k, q + 2, yd, :, B].astype(F32) + r1a[k, 1, 1, q].astype(F32)
            ).astype(BF)

        return [
            remote(g.at[k, zu, :, :, A], r1b.at[k, 0, 0], up_z),
            remote(g.at[k, zd, :, :, A], r1b.at[k, 0, 1], dn_z),
            remote(g.at[k, :, yu, :, B], r1b.at[k, 1, 0], up_y),
            remote(g.at[k, :, yd, :, B], r1b.at[k, 1, 1], dn_y),
        ]

    def s2a(k):
        @pl.loop(0, RING)
        def _(q):
            a = g[k, z, q, :, A].astype(F32) + r1b[k, 0, 0, q].astype(F32) + r1b[k, 0, 1, q].astype(F32)
            g[k, z, q, :, A] = a.astype(BF)
            b = g[k, q, y, :, B].astype(F32) + r1b[k, 1, 0, q].astype(F32) + r1b[k, 1, 1, q].astype(F32)
            g[k, q, y, :, B] = b.astype(BF)

        z2, y2 = turn(z, 2), turn(y, 2)
        return [
            remote(g.at[k, z, y2, pl.ds(0, hs), A], r2a.at[k, 0, 0], up_y),
            remote(g.at[k, z, y2, pl.ds(hs, hs), A], r2a.at[k, 0, 1], dn_y),
            remote(g.at[k, z2, y, pl.ds(0, hs), B], r2a.at[k, 1, 0], up_z),
            remote(g.at[k, z2, y, pl.ds(hs, hs), B], r2a.at[k, 1, 1], dn_z),
        ]

    def s2b(k):
        zu, zd, yu, yd = turn(z, 1), turn(z, 3), turn(y, 1), turn(y, 3)
        lo, hi = pl.ds(0, hs), pl.ds(hs, hs)
        g[k, z, yu, lo, A] = (g[k, z, yu, lo, A].astype(F32) + r2a[k, 0, 0].astype(F32)).astype(BF)
        g[k, z, yd, hi, A] = (g[k, z, yd, hi, A].astype(F32) + r2a[k, 0, 1].astype(F32)).astype(BF)
        g[k, zu, y, lo, B] = (g[k, zu, y, lo, B].astype(F32) + r2a[k, 1, 0].astype(F32)).astype(BF)
        g[k, zd, y, hi, B] = (g[k, zd, y, hi, B].astype(F32) + r2a[k, 1, 1].astype(F32)).astype(BF)
        return [
            remote(g.at[k, z, yu, :, A], r2b.at[k, 0, 0], up_y),
            remote(g.at[k, z, yd, :, A], r2b.at[k, 0, 1], dn_y),
            remote(g.at[k, zu, y, :, B], r2b.at[k, 1, 0], up_z),
            remote(g.at[k, zd, y, :, B], r2b.at[k, 1, 1], dn_z),
        ]

    def s2c(k):
        a = g[k, z, y, :, A].astype(F32) + r2b[k, 0, 0].astype(F32) + r2b[k, 0, 1].astype(F32)
        b = g[k, z, y, :, B].astype(F32) + r2b[k, 1, 0].astype(F32) + r2b[k, 1, 1].astype(F32)
        fin[k, :, A] = a
        fin[k, :, B] = b
        sq = a * a + b * b
        sq = sq.reshape(sub // 8, 8, hl).sum(0)
        total = sq[:, 0:128]
        for i in range(1, hl // 128):
            total = total + sq[:, i * 128 : (i + 1) * 128]
        return total

    def hand_over(kind):
        pex[kind] = fin[2 * other + kind].astype(BF)
        return remote(pex.at[kind], prx.at[kind], pair)

    for copy in own_w:
        copy.wait()
    give[0].wait_recv()
    c1a = {0: g1a(0)}
    wait_all(c1a[0])
    c1b = {0: g1b(0)}
    c1a[2] = g1a(2)
    give[1].wait_recv()
    c1a[1] = g1a(1)
    c1a[3] = g1a(3)
    wait_all(c1b[0])
    c2a = {0: g2a(0)}
    c2b = {}
    wait_all(c1a[1])
    c1b[1] = g1b(1)
    wait_all(c1a[2])
    c1b[2] = g1b(2)
    wait_all(c1a[3])
    c1b[3] = g1b(3)
    wait_all(c1b[1])
    c2a[1] = g2a(1)
    wait_all(c2a[0])
    c2b[0] = g2b(0)
    wait_all(c1b[2])
    c2a[2] = g2a(2)
    for copy in loads["x"]:
        copy.wait()
    wait_all(c2b[0])
    project(x0, 0, 0)
    p0 = scatter_units(0)
    wait_all(c2a[1])
    c2b[1] = g2b(1)
    wait_all(c1b[3])
    c2a[3] = g2a(3)
    wait_all(p0)
    pre0 = units_sum(0)
    pre_keep[0] = pre0
    a0 = spread_units(act.at[0], jax.nn.silu(pre0).astype(BF))
    wait_all(c2a[2])
    c2b[2] = g2b(2)
    wait_all(a0)
    wait_all(c2b[1])
    widen(x0, act.at[0], 1, x1)
    wait_all(c2b[2])
    project(x1, 2, 1)
    p1 = scatter_units(1)
    wait_all(c2a[3])
    c2b[3] = g2b(3)
    wait_all(p1)
    pre1 = units_sum(1)
    pre_keep[1] = pre1
    a1 = spread_units(act.at[1], jax.nn.silu(pre1).astype(BF))
    for copy in loads["cot"]:
        copy.wait()
    wait_all(c2b[3])
    project(cot, 3, 2)
    p2 = scatter_units(2)
    wait_all(a1)
    weight_grad(cot, act.at[1], 3)
    d1a = {3: s1a(3)}
    wait_all(p2)
    v1 = spread_units(slope.at[1], slope_of(units_sum(2), pre_keep[1]))
    d1b, d2a, d2b = {}, {}, {}
    wait_all(d1a[3])
    d1b[3] = s1b(3)
    wait_all(v1)
    weight_grad(x1, slope.at[1], 2)
    d1a[2] = s1a(2)
    widen(cot, slope.at[1], 2, err1)
    project(err1, 1, 3)
    p3 = scatter_units(3)
    weight_grad(err1, act.at[0], 1)
    d1a[1] = s1a(1)
    wait_all(p3)
    v0 = spread_units(slope.at[0], slope_of(units_sum(3), pre_keep[0]))
    wait_all(d1a[2])
    d1b[2] = s1b(2)
    wait_all(v0)
    weight_grad(x0, slope.at[0], 0)
    d1a[0] = s1a(0)
    wait_all(d1b[3])
    d2a[3] = s2a(3)
    wait_all(d1a[1])
    d1b[1] = s1b(1)
    wait_all(d2a[3])
    d2b[3] = s2b(3)
    wait_all(d1b[2])
    d2a[2] = s2a(2)
    wait_all(d1a[0])
    d1b[0] = s1b(0)
    wait_all(d2b[3])
    squares = s2c(3)
    wait_all(d2a[2])
    d2b[2] = s2b(2)
    wait_all(d1b[1])
    d2a[1] = s2a(1)
    wait_all(d2b[2])
    squares = squares + s2c(2)
    wait_all(d2a[1])
    d2b[1] = s2b(1)
    wait_all(d1b[0])
    d2a[0] = s2a(0)
    wait_all(d2b[1])
    squares = squares + s2c(1)
    h1 = hand_over(1)
    wait_all(d2a[0])
    d2b[0] = s2b(0)
    wait_all(d2b[0])
    squares = squares + s2c(0)
    h0 = hand_over(0)

    nsum[0] = squares
    nzc = [remote(nsum.at[0], nz.at[d], {"z": turn(z, d)}) for d in range(1, RING)]
    wait_all(nzc)
    nsum[1] = nsum[0] + nz[1] + nz[2] + nz[3]
    nyc = [remote(nsum.at[1], ny.at[d], {"y": turn(y, d)}) for d in range(1, RING)]
    wait_all(nyc)
    nsum[2] = nsum[1] + ny[1] + ny[2] + ny[3]
    nxc = [remote(nsum.at[2], nx.at[code], dev) for code, dev, _ in xpeers]
    wait_all(nxc)
    total = nsum[2]
    for code in range(1, GROUP):
        total = total + nx[code]
    norm = jnp.sqrt(jnp.sum(total, keepdims=True))
    norm_out[...] = jnp.broadcast_to(norm, norm_out.shape)
    factor = jnp.minimum(1.0, CLIP_NORM / norm)
    h1.wait_recv()
    h0.wait_recv()
    at_own = pl.ds(pl.multiple_of(pipe * sub, sub), sub)
    at_other = pl.ds(pl.multiple_of(other * sub, sub), sub)
    for kind, out in ((0, upd_in), (1, upd_out)):
        out[at_own, :] = fin[2 * pipe + kind] * factor
        out[at_other, :] = prx[kind].astype(F32) * factor
    for copy in started:
        copy.wait_send()


def on_device(inputs, w_in, w_out, cotangent):
    micro, tok, cols = inputs.shape
    shard, hid = w_in.shape[1], w_in.shape[2]
    sub = shard // 2
    half_d = cols // 2
    rows = micro * tok
    chunk = rows // GROUP
    hl = hid // 2
    any_spec = pl.BlockSpec(memory_space=pl.ANY)
    vmem = pl.BlockSpec(memory_space=pltpu.VMEM)
    upd_in, upd_out_t, norm = pl.pallas_call(
        kernel,
        out_shape=(
            jax.ShapeDtypeStruct((shard, hid), F32),
            jax.ShapeDtypeStruct((shard, hid), F32),
            jax.ShapeDtypeStruct((8, 128), F32),
        ),
        in_specs=[any_spec] * 4,
        out_specs=(vmem, vmem, vmem),
        scratch_shapes=[
            pltpu.VMEM((micro, tok, half_d), BF),
            pltpu.VMEM((micro, tok, half_d), BF),
            pltpu.VMEM((micro, tok, half_d), BF),
            pltpu.VMEM((micro, tok, half_d), BF),
            pltpu.VMEM((4, RING, RING, sub, hid), BF),
            pltpu.VMEM((4, RING, RING, sub, hid), BF),
            pltpu.VMEM((2, rows, hid), BF),
            pltpu.VMEM((2, rows, hid), BF),
            pltpu.VMEM((4, rows, hid), BF),
            pltpu.VMEM((4, GROUP, chunk, hid), BF),
            pltpu.VMEM((4, 2, 2, 2, sub, hl), BF),
            pltpu.VMEM((4, 2, 2, RING, sub, hl), BF),
            pltpu.VMEM((4, 2, 2, sub // 2, hl), BF),
            pltpu.VMEM((4, 2, 2, sub, hl), BF),
            pltpu.VMEM((4, sub, hid), F32),
            pltpu.VMEM((2, sub, hid), BF),
            pltpu.VMEM((2, sub, hid), BF),
            pltpu.VMEM((3, 8, 128), F32),
            pltpu.VMEM((RING, 8, 128), F32),
            pltpu.VMEM((RING, 8, 128), F32),
            pltpu.VMEM((GROUP, 8, 128), F32),
            pltpu.VMEM((2, chunk, hid), F32),
            pltpu.SemaphoreType.DMA((40,)),
            pltpu.SemaphoreType.DMA((220,)),
            pltpu.SemaphoreType.DMA((220,)),
        ],
        compiler_params=pltpu.CompilerParams(
            collective_id=0, has_side_effects=True, vmem_limit_bytes=67043328
        ),
    )(inputs, w_in[0], w_out[0].T, cotangent)
    return upd_in[None], upd_out_t.T[None], norm[0, 0]


def solution(mesh):
    split = Mesh(mesh.devices.reshape(mesh.shape["pipe"], 2, 2, RING, RING), AXES)
    placed = (
        P(None, DP, TENSOR),
        P("pipe", TENSOR_DP, None),
        P("pipe", None, TENSOR_DP),
        P(None, DP, TENSOR),
    )
    return jax.shard_map(
        on_device,
        mesh=split,
        in_specs=placed,
        out_specs=(P("pipe", TENSOR_DP, None), P("pipe", None, TENSOR_DP), P()),
        check_vma=False,
    )
```

```python
import jax
import jax.numpy as jnp
from jax import lax
from jax.experimental import pallas as pl
from jax.experimental.pallas import tpu as pltpu
from jax.sharding import Mesh
from jax.sharding import PartitionSpec as P

CLIP_NORM = 16384.0
AXES = ("pipe", "xhi", "core", "z", "y")
TENSOR = ("xhi", "core")
DP = ("z", "y")
PIPE_TENSOR_DP = ("pipe", "xhi", "core", "z", "y")
TENSOR_DP = ("xhi", "core", "z", "y")
MESH = pl.DeviceIdType.MESH
BF = jnp.bfloat16
F32 = jnp.float32

RING = 4
GROUP = 8
NT = (((1,), (1,)), ((), ()))
TN = (((0,), (0,)), ((), ()))


def kernel(
    x_hbm, win_hbm, wot_hbm, cot_hbm,
    upd_in, upd_out, norm_out,
    x0, cot, x1, err1, w, g, act, slope,
    pown, psend, crecv, xs, xrecv, pre_keep,
    ra1, ra2, ra3, rb1, rb2, rb3,
    fin, pex, prx, nsum, n1, n2,
    lsem, ssem, rsem,
):
    tok2, hid = pown.shape[1], pown.shape[2]
    sub = w.shape[3]
    la = ra3.shape[-1]
    lb = hid - la
    chunk = tok2 // GROUP
    hs = sub // 2
    pipe = lax.axis_index("pipe")
    xhi = lax.axis_index("xhi")
    core = lax.axis_index("core")
    z = lax.axis_index("z")
    y = lax.axis_index("y")
    other = 1 - pipe
    u = y // 2
    s = lax.rem(y, 2)
    q = lax.rem(y + u, 2)
    v_oth = 1 - u
    y_ag = 3 - y
    y_tp = 4 * u + 1 - y
    e_me = pipe * 4 + xhi * 2 + s

    def turn(v, d):
        return lax.rem(v + d, RING)

    started = []
    count = [0]
    lcount = [0]

    def remote(src, dst, dev):
        i = count[0]
        count[0] += 1
        copy = pltpu.make_async_remote_copy(
            src_ref=src, dst_ref=dst, send_sem=ssem.at[i], recv_sem=rsem.at[i],
            device_id=dev, device_id_type=MESH,
        )
        copy.start()
        started.append(copy)
        return copy

    def local(src, dst):
        i = lcount[0]
        lcount[0] += 1
        copy = pltpu.make_async_copy(src, dst, lsem.at[i])
        copy.start()
        return copy

    def wait_all(copies):
        for copy in copies:
            copy.wait_recv()

    xpeers = []
    for code in (7, 6, 5, 4, 3, 2, 1):
        a, b, c = code // 4, (code // 2) % 2, code % 2
        p_ = other if a else pipe
        h_ = 1 - xhi if b else xhi
        y_, s_ = (y_tp, 1 - s) if c else (y, s)
        xpeers.append((code, {"pipe": p_, "xhi": h_, "y": y_}, p_ * 4 + h_ * 2 + s_))
    wide_peers = []
    for code in range(1, 16):
        d, b, c = code // 4, (code // 2) % 2, code % 2
        wide_peers.append(
            (code, {"z": turn(z, d), "y": y_ag if b else y, "core": 1 - core if c else core})
        )
    twin = {"core": 1 - core}
    pair = {"pipe": other}

    own_w = [
        local(win_hbm.at[pl.ds(pl.multiple_of(pipe * sub, sub), sub), :], w.at[2 * pipe, z, u]),
        local(wot_hbm.at[pl.ds(pl.multiple_of(pipe * sub, sub), sub), :], w.at[2 * pipe + 1, z, u]),
    ]

    def columns(zz, vv, qq):
        member = zz * RING + (qq + vv * (3 - 2 * qq))
        return pl.ds(pl.multiple_of(member * 2 * sub + pipe * sub, sub), sub)

    loads = {}
    for name, src, dst in (("x", x_hbm, x0), ("cot", cot_hbm, cot)):
        loads[name] = [
            local(src.at[:, :, columns(zz, vv, q)], dst.at[s, :, :, pl.ds((zz * 2 + vv) * sub, sub)])
            for zz in range(RING)
            for vv in range(2)
        ]

    barrier = pltpu.get_barrier_semaphore()
    peers = [dev for _, dev, _ in xpeers] + [dev for _, dev in wide_peers]
    for dev in peers:
        pl.semaphore_signal(barrier, inc=1, device_id=dev, device_id_type=MESH)
    pl.semaphore_wait(barrier, len(peers))

    give = []
    for kind, src in ((0, win_hbm), (1, wot_hbm)):
        give.append(
            remote(
                src.at[pl.ds(pl.multiple_of(other * sub, sub), sub), :],
                w.at[2 * pipe + kind, z, u],
                pair,
            )
        )
    swaps = {}
    for name, src, dst in (("x", x_hbm, x0), ("cot", cot_hbm, cot)):
        swaps[name] = [
            remote(
                src.at[:, :, columns(zz, vv, 1 - q)],
                dst.at[s, :, :, pl.ds((zz * 2 + vv) * sub, sub)],
                {"y": y_tp},
            )
            for zz in range(RING)
            for vv in range(2)
        ]

    A, B = pl.ds(0, la), pl.ds(la, lb)
    up, dn, ag = {"z": turn(z, 1)}, {"z": turn(z, 3)}, {"y": y_ag}
    zu, zd, z2 = turn(z, 1), turn(z, 3), turn(z, 2)
    lo, hi = pl.ds(0, hs), pl.ds(hs, hs)

    def same(ref, dev):
        return remote(ref, ref, dev)

    def ga1(k):
        return [same(w.at[k, z, u, :, A], ag)]

    def ga2(k):
        ref = w.at[k, z, :, :, A]
        return [same(ref, up), same(ref, dn)]

    def ga3(k):
        return [same(w.at[k, zd, 0, :, A], up), same(w.at[k, zu, 1, :, A], dn)]

    def gb1(k):
        ref = w.at[k, z, u, :, B]
        return [same(ref, up), same(ref, dn)]

    def gb2(k):
        return [same(w.at[k, zd, u, lo, B], up), same(w.at[k, zu, u, hi, B], dn)]

    def gb3(k):
        return [same(w.at[k, :, u, :, B], ag)]

    tile = 256

    def project(src, k, ph):
        def half(which, emit):
            @pl.loop(0, hid // tile)
            def _(n):
                cols = pl.ds(pl.multiple_of(n * tile, tile), tile)
                left = src[which].reshape(tok2, src.shape[-1])
                right = w[k, :, :, :, cols].reshape(src.shape[-1], tile)
                emit(cols, jnp.dot(left, right, preferred_element_type=F32))

        def emit_send(cols, value):
            psend[ph, :, cols] = value.astype(BF)

        def emit_own(cols, value):
            pown[ph, :, cols] = value

        half(1 - core, emit_send)
        copy = remote(psend.at[ph], crecv.at[ph], twin)
        half(core, emit_own)
        return copy

    def widen(base, units, k, out):
        @pl.loop(0, RING)
        def _(zz):
            cols = pl.ds(pl.multiple_of(zz * 2 * sub, 2 * sub), 2 * sub)
            left = units[...].reshape(2 * tok2, hid)
            right = w[k, zz].reshape(2 * sub, hid)
            add = lax.dot_general(left, right, NT, preferred_element_type=F32)
            old = base[:, :, :, cols].reshape(2 * tok2, 2 * sub).astype(F32)
            out[:, :, :, cols] = (old + add).astype(BF).reshape(2, 2, tok2 // 2, 2 * sub)

    def weight_grad(left_ref, right, k):
        @pl.loop(0, RING)
        def _(zz):
            cols = pl.ds(pl.multiple_of(zz * 2 * sub, 2 * sub), 2 * sub)
            left = left_ref[:, :, :, cols].reshape(2 * tok2, 2 * sub)
            units = right[...].reshape(2 * tok2, hid)
            got = lax.dot_general(left, units, TN, preferred_element_type=F32)
            g[k, zz] = got.astype(BF).reshape(2, sub, hid)

    def scatter_units(ph, copy):
        copy.wait_recv()
        copies = []
        for code, dev, e in xpeers:
            at = pl.ds(pl.multiple_of(e * chunk, chunk), chunk)
            xs[ph, code] = (pown[ph, at, :] + crecv[ph, at, :].astype(F32)).astype(BF)
            copies.append(remote(xs.at[ph, code], xrecv.at[ph, code], dev))
        return copies

    mine = pl.ds(pl.multiple_of(e_me * chunk, chunk), chunk)

    def units_sum(ph):
        total = pown[ph, mine, :] + crecv[ph, mine, :].astype(F32)
        for code in range(1, GROUP):
            total = total + xrecv[ph, code].astype(F32)
        return total

    def spread_units(ref, value):
        ref[core, mine, :] = value
        at = ref.at[core, mine, :]
        return [remote(at, at, dev) for _, dev, _ in xpeers]

    def spread_core(ref, copies):
        wait_all(copies)
        return [same(ref.at[core], twin)]

    def slope_of(upward, pre):
        sig = jax.nn.sigmoid(pre)
        return (upward * sig * (1.0 + pre * (1.0 - sig))).astype(BF)

    def plus(x, *more):
        total = x.astype(F32)
        for m in more:
            total = total + m.astype(F32)
        return total

    def sa1(k):
        return [
            remote(g.at[k, z2, 0, :, A], ra1.at[k, 0], up),
            remote(g.at[k, z2, 1, :, A], ra1.at[k, 1], dn),
        ]

    def sa2(k):
        g[k, zu, 0, :, A] = plus(g[k, zu, 0, :, A], ra1[k, 0]).astype(BF)
        g[k, zd, 1, :, A] = plus(g[k, zd, 1, :, A], ra1[k, 1]).astype(BF)
        return [
            remote(g.at[k, zu, :, :, A], ra2.at[k, 0], up),
            remote(g.at[k, zd, :, :, A], ra2.at[k, 1], dn),
        ]

    def sa3(k):
        g[k, z, v_oth, :, A] = plus(g[k, z, v_oth, :, A], ra2[k, 0, v_oth], ra2[k, 1, v_oth]).astype(BF)
        return [remote(g.at[k, z, v_oth, :, A], ra3.at[k], ag)]

    def sb1(k):
        return [remote(g.at[k, :, v_oth, :, B], rb1.at[k], ag)]

    def sb2(k):
        @pl.loop(0, RING)
        def _(zz):
            g[k, zz, u, :, B] = plus(g[k, zz, u, :, B], rb1[k, zz]).astype(BF)

        return [
            remote(g.at[k, z2, u, lo, B], rb2.at[k, 0], up),
            remote(g.at[k, z2, u, hi, B], rb2.at[k, 1], dn),
        ]

    def sb3(k):
        g[k, zu, u, lo, B] = plus(g[k, zu, u, lo, B], rb2[k, 0]).astype(BF)
        g[k, zd, u, hi, B] = plus(g[k, zd, u, hi, B], rb2[k, 1]).astype(BF)
        return [
            remote(g.at[k, zu, u, :, B], rb3.at[k, 0], up),
            remote(g.at[k, zd, u, :, B], rb3.at[k, 1], dn),
        ]

    def fold(value):
        lanes = value.shape[-1]
        value = value.reshape(sub // 8, 8, lanes).sum(0)
        total = value[:, 0:128]
        for i in range(1, lanes // 128):
            total = total + value[:, i * 128 : (i + 1) * 128]
        return total

    def finish(k):
        a = plus(g[k, z, u, :, A], ra2[k, 0, u], ra2[k, 1, u], ra3[k])
        fin[k, :, A] = a
        b = plus(g[k, z, u, :, B], rb3[k, 0], rb3[k, 1])
        fin[k, :, B] = b
        return fold(a * a) + fold(b * b)

    def hand_over(kind):
        pex[kind] = fin[2 * other + kind].astype(BF)
        return remote(pex.at[kind], prx.at[kind], pair)

    ca1, ca2, ca3, cb1, cb2, cb3 = {}, {}, {}, {}, {}, {}
    for copy in own_w:
        copy.wait()
    give[0].wait_recv()
    ca1[0], cb1[0] = ga1(0), gb1(0)
    ca1[2], cb1[2] = ga1(2), gb1(2)
    wait_all(ca1[0])
    ca2[0] = ga2(0)
    wait_all(cb1[0])
    cb2[0] = gb2(0)
    wait_all(cb2[0])
    cb3[0] = gb3(0)
    give[1].wait_recv()
    ca1[1], cb1[1] = ga1(1), gb1(1)
    ca1[3], cb1[3] = ga1(3), gb1(3)
    wait_all(ca2[0])
    ca3[0] = ga3(0)
    wait_all(cb1[2])
    cb2[2] = gb2(2)
    wait_all(cb1[1])
    cb2[1] = gb2(1)
    wait_all(ca1[1])
    ca2[1] = ga2(1)
    for copy in loads["x"]:
        copy.wait()
    wait_all(swaps["x"])
    wait_all(ca3[0])
    wait_all(cb3[0])
    cp0 = project(x0, 0, 0)
    wait_all(cb2[1])
    cb3[1] = gb3(1)
    p0 = scatter_units(0, cp0)
    wait_all(ca2[1])
    ca3[1] = ga3(1)
    wait_all(ca1[2])
    ca2[2] = ga2(2)
    wait_all(cb2[2])
    cb3[2] = gb3(2)
    wait_all(cb1[3])
    cb2[3] = gb2(3)
    wait_all(p0)
    pre0 = units_sum(0)
    pre_keep[0] = pre0
    a0 = spread_units(act.at[0], jax.nn.silu(pre0).astype(BF))
    wait_all(ca2[2])
    ca3[2] = ga3(2)
    wait_all(ca1[3])
    ca2[3] = ga2(3)
    wait_all(cb2[3])
    cb3[3] = gb3(3)
    a0 = spread_core(act.at[0], a0)
    wait_all(ca3[1])
    wait_all(cb3[1])
    wait_all(a0)
    widen(x0, act.at[0], 1, x1)
    wait_all(ca3[2])
    wait_all(cb3[2])
    cp1 = project(x1, 2, 1)
    p1 = scatter_units(1, cp1)
    wait_all(ca2[3])
    ca3[3] = ga3(3)
    for copy in loads["cot"]:
        copy.wait()
    wait_all(swaps["cot"])
    wait_all(p1)
    pre1 = units_sum(1)
    pre_keep[1] = pre1
    a1 = spread_units(act.at[1], jax.nn.silu(pre1).astype(BF))
    wait_all(ca3[3])
    wait_all(cb3[3])
    cp2 = project(cot, 3, 2)
    p2 = scatter_units(2, cp2)
    a1 = spread_core(act.at[1], a1)
    wait_all(a1)
    weight_grad(cot, act.at[1], 3)
    da1, da2, da3, db1, db2, db3 = {}, {}, {}, {}, {}, {}
    da1[3], db1[3] = sa1(3), sb1(3)
    wait_all(p2)
    v1 = spread_units(slope.at[1], slope_of(units_sum(2), pre_keep[1]))
    wait_all(da1[3])
    da2[3] = sa2(3)
    wait_all(db1[3])
    db2[3] = sb2(3)
    v1 = spread_core(slope.at[1], v1)
    wait_all(v1)
    widen(cot, slope.at[1], 2, err1)
    cp3 = project(err1, 1, 3)
    p3 = scatter_units(3, cp3)
    weight_grad(x1, slope.at[1], 2)
    da1[2], db1[2] = sa1(2), sb1(2)
    weight_grad(err1, act.at[0], 1)
    da1[1], db1[1] = sa1(1), sb1(1)
    wait_all(p3)
    v0 = spread_units(slope.at[0], slope_of(units_sum(3), pre_keep[0]))
    wait_all(db2[3])
    db3[3] = sb3(3)
    wait_all(da2[3])
    da3[3] = sa3(3)
    wait_all(da1[2])
    da2[2] = sa2(2)
    wait_all(db1[2])
    db2[2] = sb2(2)
    v0 = spread_core(slope.at[0], v0)
    wait_all(v0)
    weight_grad(x0, slope.at[0], 0)
    da1[0], db1[0] = sa1(0), sb1(0)
    wait_all(da1[1])
    da2[1] = sa2(1)
    wait_all(db1[1])
    db2[1] = sb2(1)
    wait_all(db2[2])
    db3[2] = sb3(2)
    wait_all(da2[2])
    da3[2] = sa3(2)
    wait_all(da3[3])
    wait_all(db3[3])
    squares = finish(3)
    wait_all(da1[0])
    da2[0] = sa2(0)
    wait_all(db1[0])
    db2[0] = sb2(0)
    wait_all(db2[1])
    db3[1] = sb3(1)
    wait_all(da2[1])
    da3[1] = sa3(1)
    wait_all(db2[0])
    db3[0] = sb3(0)
    wait_all(da3[2])
    wait_all(db3[2])
    squares = squares + finish(2)
    wait_all(da2[0])
    da3[0] = sa3(0)
    wait_all(da3[1])
    wait_all(db3[1])
    squares = squares + finish(1)
    h1 = hand_over(1)
    wait_all(da3[0])
    wait_all(db3[0])
    squares = squares + finish(0)
    nsum[0] = squares
    c1 = [remote(nsum.at[0], n1.at[code], dev) for code, dev, _ in xpeers]
    h0 = hand_over(0)
    wait_all(c1)
    total = nsum[0]
    for code in range(1, GROUP):
        total = total + n1[code]
    nsum[1] = total
    c2 = [remote(nsum.at[1], n2.at[code], dev) for code, dev in wide_peers]
    wait_all(c2)
    total = nsum[1]
    for code in range(1, 16):
        total = total + n2[code]
    norm = jnp.sqrt(jnp.sum(total, keepdims=True))
    norm_out[...] = jnp.broadcast_to(norm, norm_out.shape)
    factor = jnp.minimum(1.0, CLIP_NORM / norm)
    h1.wait_recv()
    h0.wait_recv()
    at_own = pl.ds(pl.multiple_of(pipe * sub, sub), sub)
    at_other = pl.ds(pl.multiple_of(other * sub, sub), sub)
    for kind, out in ((0, upd_in), (1, upd_out)):
        out[at_own, :] = fin[2 * pipe + kind] * factor
        out[at_other, :] = prx[kind].astype(F32) * factor
    for copy in started:
        copy.wait_send()


def on_device(inputs, w_in, w_out, cotangent):
    micro, tok, cols = inputs.shape
    shard, hid = w_in.shape[1], w_in.shape[2]
    sub = shard // 2
    part_d = cols // 4
    rows = micro * tok
    chunk = rows // GROUP
    la = 5 * hid // 8
    lb = hid - la
    any_spec = pl.BlockSpec(memory_space=pl.ANY)
    vmem = pl.BlockSpec(memory_space=pltpu.VMEM)
    upd_in, upd_out_t, norm = pl.pallas_call(
        kernel,
        out_shape=(
            jax.ShapeDtypeStruct((shard, hid), F32),
            jax.ShapeDtypeStruct((shard, hid), F32),
            jax.ShapeDtypeStruct((8, 128), F32),
        ),
        in_specs=[any_spec] * 4,
        out_specs=(vmem, vmem, vmem),
        scratch_shapes=[
            pltpu.VMEM((2, micro, tok, part_d), BF),
            pltpu.VMEM((2, micro, tok, part_d), BF),
            pltpu.VMEM((2, micro, tok, part_d), BF),
            pltpu.VMEM((2, micro, tok, part_d), BF),
            pltpu.VMEM((4, RING, 2, sub, hid), BF),
            pltpu.VMEM((4, RING, 2, sub, hid), BF),
            pltpu.VMEM((2, 2, rows, hid), BF),
            pltpu.VMEM((2, 2, rows, hid), BF),
            pltpu.VMEM((4, rows, hid), F32),
            pltpu.VMEM((4, rows, hid), BF),
            pltpu.VMEM((4, rows, hid), BF),
            pltpu.VMEM((4, GROUP, chunk, hid), BF),
            pltpu.VMEM((4, GROUP, chunk, hid), BF),
            pltpu.VMEM((2, chunk, hid), F32),
            pltpu.VMEM((4, 2, sub, la), BF),
            pltpu.VMEM((4, 2, 2, sub, la), BF),
            pltpu.VMEM((4, sub, la), BF),
            pltpu.VMEM((4, RING, sub, lb), BF),
            pltpu.VMEM((4, 2, sub // 2, lb), BF),
            pltpu.VMEM((4, 2, sub, lb), BF),
            pltpu.VMEM((4, sub, hid), F32),
            pltpu.VMEM((2, sub, hid), BF),
            pltpu.VMEM((2, sub, hid), BF),
            pltpu.VMEM((2, 8, 128), F32),
            pltpu.VMEM((GROUP, 8, 128), F32),
            pltpu.VMEM((16, 8, 128), F32),
            pltpu.SemaphoreType.DMA((20,)),
            pltpu.SemaphoreType.DMA((200,)),
            pltpu.SemaphoreType.DMA((200,)),
        ],
        compiler_params=pltpu.CompilerParams(
            collective_id=0, has_side_effects=True, vmem_limit_bytes=67043328
        ),
    )(inputs, w_in[0], w_out[0].T, cotangent)
    return upd_in[None], upd_out_t.T[None], norm[0, 0]


def solution(mesh):
    split = Mesh(mesh.devices.reshape(mesh.shape["pipe"], 2, 2, RING, RING), AXES)
    placed = (
        P(None, DP, TENSOR),
        P("pipe", TENSOR_DP, None),
        P("pipe", None, TENSOR_DP),
        P(None, DP, TENSOR),
    )
    return jax.shard_map(
        on_device,
        mesh=split,
        in_specs=placed,
        out_specs=(P("pipe", TENSOR_DP, None), P("pipe", None, TENSOR_DP), P()),
        check_vma=False,
    )
```

```python
import jax
import jax.numpy as jnp
from jax import lax
from jax.experimental import pallas as pl
from jax.experimental.pallas import tpu as pltpu
from jax.sharding import Mesh
from jax.sharding import PartitionSpec as P

CLIP_NORM = 16384.0
AXES = ("pipe", "xhi", "core", "z", "y")
TENSOR = ("xhi", "core")
DP = ("z", "y")
PIPE_TENSOR_DP = ("pipe", "xhi", "core", "z", "y")
TENSOR_DP = ("xhi", "core", "z", "y")
MESH = pl.DeviceIdType.MESH
BF = jnp.bfloat16
F32 = jnp.float32

RING = 4
NT = (((1,), (1,)), ((), ()))
TN = (((0,), (0,)), ((), ()))


def kernel(
    x_hbm, win_hbm, wot_hbm, cot_hbm,
    upd_in, upd_out, norm_out,
    stage, x0, cot, x1, err1, own, w, g, act, slope,
    part, r1, r2, keep,
    rc, ra, rb,
    fin, pex, prx, nsum, n1, n2,
    lsem, ssem, rsem,
):
    group, hid = part.shape[2], part.shape[3]
    rows = RING * group
    sub = w.shape[3]
    hl = hid // 2
    chunk = group // RING
    hs = sub // 2
    part_d = x0.shape[-1]
    tile = 256
    pipe = lax.axis_index("pipe")
    xhi = lax.axis_index("xhi")
    core = lax.axis_index("core")
    z = lax.axis_index("z")
    y = lax.axis_index("y")
    other = 1 - pipe
    core2 = 1 - core
    xi = xhi * 2 + pipe

    def turn(v, d):
        return lax.rem(v + d, RING)

    started = []
    count = [0]
    lcount = [0]

    def remote(src, dst, dev):
        i = count[0]
        count[0] += 1
        copy = pltpu.make_async_remote_copy(
            src_ref=src, dst_ref=dst, send_sem=ssem.at[i], recv_sem=rsem.at[i],
            device_id=dev, device_id_type=MESH,
        )
        copy.start()
        started.append(copy)
        return copy

    def same(ref, dev):
        return remote(ref, ref, dev)

    def local(src, dst):
        i = lcount[0]
        lcount[0] += 1
        copy = pltpu.make_async_copy(src, dst, lsem.at[i])
        copy.start()
        return copy

    def wait_all(copies):
        for copy in copies:
            copy.wait_recv()

    xpeers = []
    for code in (3, 2, 1):
        p_ = other if code % 2 else pipe
        h_ = 1 - xhi if code // 2 else xhi
        xpeers.append((code, {"pipe": p_, "xhi": h_}, h_ * 2 + p_))
    ypeers = [(d, {"y": turn(y, d)}, turn(y, d)) for d in (2, 1, 3)]
    zpeers = [(d, {"z": turn(z, d)}) for d in (1, 2, 3)]
    up, dn = {"z": turn(z, 1)}, {"z": turn(z, 3)}
    zu, zd, z2 = turn(z, 1), turn(z, 3), turn(z, 2)
    twin = {"core": core2}
    pair = {"pipe": other}
    ycore = [(d * 2, {**dev}, yy, core) for d, dev, yy in ypeers]
    ycore += [(d * 2 + 1, {**dev, "core": core2}, yy, core2) for d, dev, yy in ypeers]
    ycore += [(1, twin, y, core2)]
    xz = [(code, dev) for code, dev, _ in xpeers]
    xz += [(d * 4, dev) for d, dev in zpeers]
    xz += [(d * 4 + code, {**dx, **dz}) for d, dz in zpeers for code, dx, _ in xpeers]

    keep_rows = pl.ds(pl.multiple_of(pipe * sub, sub), sub)
    give_rows = pl.ds(pl.multiple_of(other * sub, sub), sub)
    own_load = [
        local(win_hbm.at[give_rows, :], own.at[0]),
        local(wot_hbm.at[give_rows, :], own.at[1]),
        local(win_hbm.at[keep_rows, :], w.at[2 * pipe, core, z]),
        local(wot_hbm.at[keep_rows, :], w.at[2 * pipe + 1, core, z]),
    ]

    def fetch(src, n):
        copies = []
        for yy in range(RING):
            for zz in range(RING):
                off = pl.multiple_of((zz * RING + yy) * 2 * sub + pipe * sub, sub)
                copies.append(
                    local(src.at[:, :, pl.ds(off, sub)], stage.at[n, yy, :, :, pl.ds(zz * sub, sub)])
                )
        return copies

    x_load = fetch(x_hbm, 0)
    cot_load = fetch(cot_hbm, 1)

    barrier = pltpu.get_barrier_semaphore()
    peers = [dev for _, dev, _, _ in ycore] + [dev for _, dev in xz]
    for dev in peers:
        pl.semaphore_signal(barrier, inc=1, device_id=dev, device_id_type=MESH)
    pl.semaphore_wait(barrier, len(peers))

    half_tok = x0.shape[2]
    my_cols = pl.ds(pl.multiple_of(core * (part_d // 2), part_d // 2), part_d // 2)

    def swap_tokens(n, dst):
        def piece(yy, cc):
            toks = pl.ds(pl.multiple_of(cc * half_tok, half_tok), half_tok)
            return stage.at[n, yy, :, toks, :]

        landing = dst.at[y, :, :, my_cols]
        return local(piece(y, core), landing), [
            remote(piece(yy, cc), landing, dev) for _, dev, yy, cc in ycore
        ]

    lo, hi = pl.ds(0, hs), pl.ds(hs, hs)

    def g1(k):
        ref = w.at[k, core, z]
        return [same(ref, up), same(ref, dn)]

    def g2(k):
        ring = [same(w.at[k, core, zd, lo, :], up), same(w.at[k, core, zu, hi, :], dn)]
        return ring, [same(w.at[k, core, at], twin) for at in (z, zu, zd)]

    def g3(k):
        return [same(w.at[k, core, z2], twin)]

    halves = (pl.ds(0, hl), pl.ds(hl, hl))

    def project(src, k, ph, half):
        @pl.loop(0, hl // tile)
        def _(n):
            cols = pl.ds(pl.multiple_of(half * hl + n * tile, tile), tile)
            left = src[...].reshape(rows, part_d)
            right = w[k, :, :, :, cols].reshape(part_d, tile)
            got = jnp.dot(left, right, preferred_element_type=F32)
            part[ph, :, :, cols] = got.astype(BF).reshape(RING, group, tile)

    def widen(base, units, k, out):
        for cc in range(2):
            @pl.loop(0, 2)
            def _(p):
                cols = pl.ds(pl.multiple_of(cc * RING * sub + p * 2 * sub, tile), 2 * sub)
                left = units[...].reshape(rows, hid)
                right = w[k, cc, pl.ds(p * 2, 2)].reshape(2 * sub, hid)
                add = lax.dot_general(left, right, NT, preferred_element_type=F32)
                old = base[:, :, :, cols].reshape(rows, 2 * sub).astype(F32)
                out[:, :, :, cols] = (old + add).astype(BF).reshape(RING, 2, half_tok, 2 * sub)

    def weight_grad(left_ref, right, k):
        def side(cc):
            @pl.loop(0, 2)
            def _(p):
                cols = pl.ds(pl.multiple_of(cc * RING * sub + p * 2 * sub, tile), 2 * sub)
                left = left_ref[:, :, :, cols].reshape(rows, 2 * sub)
                units = right[...].reshape(rows, hid)
                got = lax.dot_general(left, units, TN, preferred_element_type=F32)
                g[k, cc, pl.ds(p * 2, 2)] = got.astype(BF).reshape(2, sub, hid)

        side(core2)
        copy = remote(g.at[k, core2], rc.at[k], twin)
        side(core)
        return [copy]

    def plus(x, *more):
        total = x.astype(F32)
        for m in more:
            total = total + m.astype(F32)
        return total

    first = (xpeers, ypeers)
    second = (ypeers, xpeers)
    block = (xi, y)
    inner = (y, xi)

    def inner_rows(at):
        return pl.ds(pl.multiple_of(at * chunk, chunk), chunk)

    def rs1(ph, half):
        lanes = halves[half]
        return [
            remote(part.at[ph, at, :, lanes], r1.at[ph, half, slot], dev)
            for slot, dev, at in first[half]
        ]

    def rs2(ph, half, copies):
        wait_all(copies)
        lanes = halves[half]
        b = block[half]
        part[ph, b, :, lanes] = plus(
            part[ph, b, :, lanes], r1[ph, half, 1], r1[ph, half, 2], r1[ph, half, 3]
        ).astype(BF)
        return [
            remote(part.at[ph, b, inner_rows(at), lanes], r2.at[ph, half, slot], dev)
            for slot, dev, at in second[half]
        ]

    def units(ph, half, copies):
        wait_all(copies)
        return plus(
            part[ph, block[half], inner_rows(inner[half]), halves[half]],
            r2[ph, half, 1], r2[ph, half, 2], r2[ph, half, 3],
        )

    def sp1(ref, half, value):
        b, at, lanes = block[half], inner_rows(inner[half]), halves[half]
        ref[b, at, lanes] = value
        piece = ref.at[b, at, lanes]
        return [same(piece, dev) for _, dev, _ in second[half]]

    def sp2(ref, half, copies):
        wait_all(copies)
        piece = ref.at[block[half], :, halves[half]]
        return [same(piece, dev) for _, dev, _ in first[half]]

    def slope_of(upward, pre):
        sig = jax.nn.sigmoid(pre)
        return (upward * sig * (1.0 + pre * (1.0 - sig))).astype(BF)

    def q1(k, copies):
        wait_all(copies)
        g[k, core, z2] = plus(g[k, core, z2], rc[k, z2]).astype(BF)
        return [
            remote(g.at[k, core, z2, lo, :], ra.at[k, 0], up),
            remote(g.at[k, core, z2, hi, :], ra.at[k, 1], dn),
        ]

    def q2(k, copies):
        g[k, core, zu, hi, :] = plus(g[k, core, zu, hi, :], rc[k, zu, hi, :]).astype(BF)
        g[k, core, zd, lo, :] = plus(g[k, core, zd, lo, :], rc[k, zd, lo, :]).astype(BF)
        wait_all(copies)
        g[k, core, zu, lo, :] = plus(g[k, core, zu, lo, :], rc[k, zu, lo, :], ra[k, 0]).astype(BF)
        g[k, core, zd, hi, :] = plus(g[k, core, zd, hi, :], rc[k, zd, hi, :], ra[k, 1]).astype(BF)
        return [
            remote(g.at[k, core, zu], rb.at[k, 0], up),
            remote(g.at[k, core, zd], rb.at[k, 1], dn),
        ]

    def fold(value):
        lanes = value.shape[-1]
        value = value.reshape(sub // 8, 8, lanes).sum(0)
        total = value[:, 0:128]
        for i in range(1, lanes // 128):
            total = total + value[:, i * 128 : (i + 1) * 128]
        return total

    def finish(k, copies):
        wait_all(copies)
        value = plus(g[k, core, z], rc[k, z], rb[k, 0], rb[k, 1])
        fin[k] = value
        return fold(value * value)

    def hand_over(kind):
        pex[kind] = fin[2 * other + kind].astype(BF)
        return remote(pex.at[kind], prx.at[kind], pair)

    for copy in own_load:
        copy.wait()
    k_own = (3 * pipe, 1 + pipe)
    k_got = (3 * other, 1 + other)
    ca0 = g1(k_own[0])
    e0 = remote(own.at[pipe], w.at[3 * pipe, core, z], pair)
    e1 = remote(own.at[other], w.at[1 + pipe, core, z], pair)
    for copy in x_load:
        copy.wait()
    x_here, x_swap = swap_tokens(0, x0)
    e0.wait_recv()
    ca1 = g1(k_got[0])
    wait_all(ca0)
    cb0, cc0 = g2(k_own[0])
    for copy in cot_load:
        copy.wait()
    cot_here, cot_swap = swap_tokens(1, cot)
    wait_all(ca1)
    cb1, cc1 = g2(k_got[0])
    ca2 = g1(k_own[1])
    e1.wait_recv()
    ca3 = g1(k_got[1])
    wait_all(cb0)
    cd0 = g3(k_own[0])
    wait_all(cb1)
    cd1 = g3(k_got[0])
    x_here.wait()
    wait_all(x_swap)
    wait_all(cc0 + cc1)
    wait_all(cd0 + cd1)
    project(x0, 0, 0, 0)
    p0a = rs1(0, 0)
    project(x0, 0, 0, 1)
    p0b = rs1(0, 1)
    wait_all(ca2)
    cb2, cc2 = g2(k_own[1])
    wait_all(ca3)
    cb3, cc3 = g2(k_got[1])
    cot_here.wait()
    wait_all(cot_swap)
    project(cot, 3, 2, 0)
    project(cot, 3, 2, 1)
    p0a = rs2(0, 0, p0a)
    p0b = rs2(0, 1, p0b)
    wait_all(cb2)
    cd2 = g3(k_own[1])
    pre = units(0, 0, p0a)
    keep[0, 0] = pre
    a0a = sp1(act.at[0], 0, jax.nn.silu(pre).astype(BF))
    pre = units(0, 1, p0b)
    keep[0, 1] = pre
    a0b = sp1(act.at[0], 1, jax.nn.silu(pre).astype(BF))
    a0a = sp2(act.at[0], 0, a0a)
    a0b = sp2(act.at[0], 1, a0b)
    p2a = rs1(2, 0)
    p2b = rs1(2, 1)
    wait_all(cb3)
    cd3 = g3(k_got[1])
    wait_all(cc2 + cc3)
    wait_all(cd2 + cd3)
    wait_all(a0a)
    wait_all(a0b)
    widen(x0, act.at[0], 1, x1)
    project(x1, 2, 1, 0)
    p1a = rs1(1, 0)
    project(x1, 2, 1, 1)
    p1b = rs1(1, 1)
    p2a = rs2(2, 0, p2a)
    p2b = rs2(2, 1, p2b)
    up1a = units(2, 0, p2a)
    keep[1, 0] = up1a
    up1b = units(2, 1, p2b)
    keep[1, 1] = up1b
    p1a = rs2(1, 0, p1a)
    p1b = rs2(1, 1, p1b)
    pre = units(1, 0, p1a)
    s1a = sp1(slope.at[1], 0, slope_of(keep[1, 0], pre))
    a1a = sp1(act.at[1], 0, jax.nn.silu(pre).astype(BF))
    pre = units(1, 1, p1b)
    s1b = sp1(slope.at[1], 1, slope_of(keep[1, 1], pre))
    a1b = sp1(act.at[1], 1, jax.nn.silu(pre).astype(BF))
    s1a = sp2(slope.at[1], 0, s1a)
    s1b = sp2(slope.at[1], 1, s1b)
    a1a = sp2(act.at[1], 0, a1a)
    a1b = sp2(act.at[1], 1, a1b)
    wait_all(s1a)
    wait_all(s1b)
    widen(cot, slope.at[1], 2, err1)
    project(err1, 1, 3, 0)
    p3a = rs1(3, 0)
    project(err1, 1, 3, 1)
    p3b = rs1(3, 1)
    d2 = weight_grad(x1, slope.at[1], 2)
    d1 = weight_grad(err1, act.at[0], 1)
    d2 = q1(2, d2)
    p3a = rs2(3, 0, p3a)
    p3b = rs2(3, 1, p3b)
    d1 = q1(1, d1)
    d2 = q2(2, d2)
    s0a = sp1(slope.at[0], 0, slope_of(units(3, 0, p3a), keep[0, 0]))
    s0b = sp1(slope.at[0], 1, slope_of(units(3, 1, p3b), keep[0, 1]))
    wait_all(a1a)
    wait_all(a1b)
    d3 = weight_grad(cot, act.at[1], 3)
    s0a = sp2(slope.at[0], 0, s0a)
    s0b = sp2(slope.at[0], 1, s0b)
    d3 = q1(3, d3)
    d1 = q2(1, d1)
    squares = finish(2, d2)
    wait_all(s0a)
    wait_all(s0b)
    d0 = weight_grad(x0, slope.at[0], 0)
    d0 = q1(0, d0)
    d3 = q2(3, d3)
    squares = squares + finish(1, d1)
    d0 = q2(0, d0)
    squares = squares + finish(3, d3)
    h1 = hand_over(1)
    squares = squares + finish(0, d0)
    nsum[0] = squares
    c1 = [remote(nsum.at[0], n1.at[code], dev) for code, dev, _, _ in ycore]
    h0 = hand_over(0)
    wait_all(c1)
    total = nsum[0]
    for code in range(1, 8):
        total = total + n1[code]
    nsum[1] = total
    c2 = [remote(nsum.at[1], n2.at[code], dev) for code, dev in xz]
    wait_all(c2)
    total = nsum[1]
    for code in range(1, 16):
        total = total + n2[code]
    norm = jnp.sqrt(jnp.sum(total, keepdims=True))
    norm_out[...] = jnp.broadcast_to(norm, norm_out.shape)
    factor = jnp.minimum(1.0, CLIP_NORM / norm)
    h1.wait_recv()
    h0.wait_recv()
    for kind, out in ((0, upd_in), (1, upd_out)):
        out[keep_rows, :] = fin[2 * pipe + kind] * factor
        out[give_rows, :] = prx[kind].astype(F32) * factor
    for copy in started:
        copy.wait_send()


def on_device(inputs, w_in, w_out, cotangent):
    micro, tok, cols = inputs.shape
    shard, hid = w_in.shape[1], w_in.shape[2]
    sub = shard // 2
    part_d = cols // 4
    group = micro * tok // 2
    hl = hid // 2
    any_spec = pl.BlockSpec(memory_space=pl.ANY)
    vmem = pl.BlockSpec(memory_space=pltpu.VMEM)
    tokens = pltpu.VMEM((RING, micro, tok // 2, part_d), BF)
    weights = pltpu.VMEM((4, 2, RING, sub, hid), BF)
    layers = pltpu.VMEM((2, RING, group, hid), BF)
    upd_in, upd_out_t, norm = pl.pallas_call(
        kernel,
        out_shape=(
            jax.ShapeDtypeStruct((shard, hid), F32),
            jax.ShapeDtypeStruct((shard, hid), F32),
            jax.ShapeDtypeStruct((8, 128), F32),
        ),
        in_specs=[any_spec] * 4,
        out_specs=(vmem, vmem, vmem),
        scratch_shapes=[
            pltpu.VMEM((2, RING, micro, tok, RING * sub), BF),
            tokens, tokens, tokens, tokens,
            pltpu.VMEM((2, sub, hid), BF),
            weights, weights, layers, layers,
            pltpu.VMEM((4, RING, group, hid), BF),
            pltpu.VMEM((4, 2, RING, group, hl), BF),
            pltpu.VMEM((4, 2, RING, group // RING, hl), BF),
            pltpu.VMEM((2, 2, group // RING, hl), F32),
            pltpu.VMEM((4, RING, sub, hid), BF),
            pltpu.VMEM((4, 2, sub // 2, hid), BF),
            pltpu.VMEM((4, 2, sub, hid), BF),
            pltpu.VMEM((4, sub, hid), F32),
            pltpu.VMEM((2, sub, hid), BF),
            pltpu.VMEM((2, sub, hid), BF),
            pltpu.VMEM((2, 8, 128), F32),
            pltpu.VMEM((8, 8, 128), F32),
            pltpu.VMEM((16, 8, 128), F32),
            pltpu.SemaphoreType.DMA((40,)),
            pltpu.SemaphoreType.DMA((200,)),
            pltpu.SemaphoreType.DMA((200,)),
        ],
        compiler_params=pltpu.CompilerParams(
            collective_id=0, has_side_effects=True, vmem_limit_bytes=67043328
        ),
    )(inputs, w_in[0], w_out[0].T, cotangent)
    return upd_in[None], upd_out_t.T[None], norm[0, 0]


def solution(mesh):
    split = Mesh(mesh.devices.reshape(mesh.shape["pipe"], 2, 2, RING, RING), AXES)
    placed = (
        P(None, DP, TENSOR),
        P("pipe", TENSOR_DP, None),
        P("pipe", None, TENSOR_DP),
        P(None, DP, TENSOR),
    )
    return jax.shard_map(
        on_device,
        mesh=split,
        in_specs=placed,
        out_specs=(P("pipe", TENSOR_DP, None), P("pipe", None, TENSOR_DP), P()),
        check_vma=False,
    )
```

```python
import jax
import jax.numpy as jnp
from jax import lax
from jax.experimental import pallas as pl
from jax.experimental.pallas import tpu as pltpu
from jax.sharding import Mesh
from jax.sharding import PartitionSpec as P

CLIP_NORM = 16384.0
AXES = ("pipe", "xhi", "core", "z", "y")
TENSOR = ("xhi", "core")
DP = ("z", "y")
PIPE_TENSOR_DP = ("pipe", "xhi", "core", "z", "y")
TENSOR_DP = ("xhi", "core", "z", "y")
MESH = pl.DeviceIdType.MESH
BF = jnp.bfloat16
F32 = jnp.float32

RING = 4
NT = (((1,), (1,)), ((), ()))
TN = (((0,), (0,)), ((), ()))


def kernel(
    x_hbm, win_hbm, wout_hbm, cot_hbm,
    tot_in, tot_out, norm_out,
    stage, x0, cot, x1, err1, raw, own, w, g, act, slope,
    part, r1, r2, keep,
    rc, ra, rb,
    fin, pex, prx, late, turned, nsum, n1, n2,
    lsem, ssem, rsem,
):
    group, hid = part.shape[2], part.shape[3]
    rows = RING * group
    sub = w.shape[3]
    hl = hid // 2
    hs = sub // 2
    part_d = x0.shape[-1]
    tile = 256
    pipe = lax.axis_index("pipe")
    xhi = lax.axis_index("xhi")
    core = lax.axis_index("core")
    z = lax.axis_index("z")
    y = lax.axis_index("y")
    other = 1 - pipe
    core2 = 1 - core
    xi = xhi * 2 + pipe

    def turn(v, d):
        return lax.rem(v + d, RING)

    started = []
    count = [0]
    lcount = [0]

    def remote(src, dst, dev):
        i = count[0]
        count[0] += 1
        copy = pltpu.make_async_remote_copy(
            src_ref=src, dst_ref=dst, send_sem=ssem.at[i], recv_sem=rsem.at[i],
            device_id=dev, device_id_type=MESH,
        )
        copy.start()
        started.append(copy)
        return copy

    def same(ref, dev):
        return remote(ref, ref, dev)

    def local(src, dst):
        i = lcount[0]
        lcount[0] += 1
        copy = pltpu.make_async_copy(src, dst, lsem.at[i])
        copy.start()
        return copy

    def wait_all(copies):
        for copy in copies:
            copy.wait_recv()

    xpeers = []
    for code in (3, 2, 1):
        p_ = other if code % 2 else pipe
        h_ = 1 - xhi if code // 2 else xhi
        xpeers.append((code, {"pipe": p_, "xhi": h_}, h_ * 2 + p_))
    ypeers = [(d, {"y": turn(y, d)}, turn(y, d)) for d in (2, 1, 3)]
    zpeers = [(d, {"z": turn(z, d)}) for d in (1, 2, 3)]
    up, dn = {"z": turn(z, 1)}, {"z": turn(z, 3)}
    zu, zd, z2 = turn(z, 1), turn(z, 3), turn(z, 2)
    twin = {"core": core2}
    pair = {"pipe": other}
    ycore = [(d * 2, {**dev}, yy, core) for d, dev, yy in ypeers]
    ycore += [(d * 2 + 1, {**dev, "core": core2}, yy, core2) for d, dev, yy in ypeers]
    ycore += [(1, twin, y, core2)]
    xz = [(code, dev) for code, dev, _ in xpeers]
    xz += [(d * 4, dev) for d, dev in zpeers]
    xz += [(d * 4 + code, {**dx, **dz}) for d, dz in zpeers for code, dx, _ in xpeers]

    keep_rows = pl.ds(pl.multiple_of(pipe * sub, sub), sub)
    give_rows = pl.ds(pl.multiple_of(other * sub, sub), sub)
    out_load = [
        local(wout_hbm.at[:, give_rows], raw.at[0]),
        local(wout_hbm.at[:, keep_rows], raw.at[1]),
    ]
    own_load = [
        local(win_hbm.at[give_rows, :], own.at[0]),
        local(win_hbm.at[keep_rows, :], w.at[2 * pipe, core, z]),
    ]

    def fetch(src, n):
        copies = []
        for yy in range(RING):
            for zz in range(RING):
                off = pl.multiple_of((zz * RING + yy) * 2 * sub + pipe * sub, sub)
                copies.append(
                    local(src.at[:, :, pl.ds(off, sub)], stage.at[n, yy, :, :, pl.ds(zz * sub, sub)])
                )
        return copies

    x_load = fetch(x_hbm, 0)
    cot_load = fetch(cot_hbm, 1)

    barrier = pltpu.get_barrier_semaphore()
    peers = [dev for _, dev, _, _ in ycore] + [dev for _, dev in xz]
    for dev in peers:
        pl.semaphore_signal(barrier, inc=1, device_id=dev, device_id_type=MESH)
    for copy in out_load:
        copy.wait()
    own[1] = raw[0].T
    w[2 * pipe + 1, core, z] = raw[1].T
    pl.semaphore_wait(barrier, len(peers))

    half_tok = x0.shape[2]
    my_cols = pl.ds(pl.multiple_of(core * (part_d // 2), part_d // 2), part_d // 2)

    def swap_tokens(n, dst):
        def piece(yy, cc):
            toks = pl.ds(pl.multiple_of(cc * half_tok, half_tok), half_tok)
            return stage.at[n, yy, :, toks, :]

        landing = dst.at[y, :, :, my_cols]
        return local(piece(y, core), landing), [
            remote(piece(yy, cc), landing, dev) for _, dev, yy, cc in ycore
        ]

    lo, hi = pl.ds(0, hs), pl.ds(hs, hs)

    def g1(k, rows_of=slice(None)):
        ref = w.at[k, core, z, rows_of, :]
        return [same(ref, up), same(ref, dn)]

    def g2(k, cuts=(lo, hi)):
        ring = [same(w.at[k, core, zd, r, :], up) for r in cuts[: len(cuts) // 2]]
        ring += [same(w.at[k, core, zu, r, :], dn) for r in cuts[len(cuts) // 2 :]]
        return ring

    def g2c(k):
        return [same(w.at[k, core, at], twin) for at in (z, zu, zd)]

    def g3(k):
        return [same(w.at[k, core, z2], twin)]

    halves = (pl.ds(0, hl), pl.ds(hl, hl))

    mrows = group // 2
    streams = (pl.ds(0, mrows), pl.ds(mrows, mrows))
    srows = RING * mrows

    def project(src, k, ph, half, m):
        @pl.loop(0, hl // tile)
        def _(n):
            cols = pl.ds(pl.multiple_of(half * hl + n * tile, tile), tile)
            left = src[:, m].reshape(srows, part_d)
            right = w[k, :, :, :, cols].reshape(part_d, tile)
            got = jnp.dot(left, right, preferred_element_type=F32)
            part[ph, :, streams[m], cols] = got.astype(BF).reshape(RING, mrows, tile)

    def widen(base, units_ref, k, out, m):
        for cc in range(2):
            @pl.loop(0, 2)
            def _(p):
                cols = pl.ds(pl.multiple_of(cc * RING * sub + p * 2 * sub, tile), 2 * sub)
                left = units_ref[:, streams[m], :].reshape(srows, hid)
                right = w[k, cc, pl.ds(p * 2, 2)].reshape(2 * sub, hid)
                add = lax.dot_general(left, right, NT, preferred_element_type=F32)
                old = base[:, m, :, cols].reshape(srows, 2 * sub).astype(F32)
                out[:, m, :, cols] = (old + add).astype(BF).reshape(RING, mrows, 2 * sub)

    def weight_grad(left_ref, right, k):
        def side(cc, p):
            zz = pl.ds(pl.multiple_of(p * 2, 2), 2)
            cols = pl.ds(pl.multiple_of(cc * RING * sub + p * 2 * sub, tile), 2 * sub)
            left = left_ref[:, :, :, cols].reshape(rows, 2 * sub)
            got = lax.dot_general(left, right[...].reshape(rows, hid), TN, preferred_element_type=F32)
            g[k, cc, zz] = got.astype(BF).reshape(2, sub, hid)

        def across(p):
            zz = pl.ds(pl.multiple_of(p * 2, 2), 2)
            return remote(g.at[k, core2, zz], rc.at[k, zz], twin)

        p_far = z2 // 2
        p_near = 1 - p_far
        side(core2, p_far)
        far = across(p_far)
        side(core2, p_near)
        near = across(p_near)
        side(core, p_far)
        sent = q1(k, [far])
        side(core, p_near)
        return sent, near

    def plus(x, *more):
        total = x.astype(F32)
        for m in more:
            total = total + m.astype(F32)
        return total

    first = (xpeers, ypeers)
    second = (ypeers, xpeers)
    block = (xi, y)
    inner = (y, xi)

    crows = mrows // RING

    def inner_rows(at, m):
        return pl.ds(pl.multiple_of(m * mrows + at * crows, crows), crows)

    def slots(m):
        return pl.ds(m * crows, crows)

    def rs1(ph, half, m):
        lanes, r = halves[half], streams[m]
        return [
            remote(part.at[ph, at, r, lanes], r1.at[ph, half, slot, r], dev)
            for slot, dev, at in first[half]
        ]

    def rs2(ph, half, m, copies):
        wait_all(copies)
        lanes, r = halves[half], streams[m]
        b = block[half]
        part[ph, b, r, lanes] = plus(
            part[ph, b, r, lanes], r1[ph, half, 1, r], r1[ph, half, 2, r], r1[ph, half, 3, r]
        ).astype(BF)
        return [
            remote(part.at[ph, b, inner_rows(at, m), lanes], r2.at[ph, half, slot, slots(m)], dev)
            for slot, dev, at in second[half]
        ]

    def units(ph, half, m, copies):
        wait_all(copies)
        c = slots(m)
        return plus(
            part[ph, block[half], inner_rows(inner[half], m), halves[half]],
            r2[ph, half, 1, c], r2[ph, half, 2, c], r2[ph, half, 3, c],
        )

    def put(ref, half, m, value):
        ref[block[half], inner_rows(inner[half], m), halves[half]] = value

    def sp1(ref, half, m):
        piece = ref.at[block[half], inner_rows(inner[half], m), halves[half]]
        return [same(piece, dev) for _, dev, _ in second[half]]

    def sp2(ref, half, m, copies):
        wait_all(copies)
        piece = ref.at[block[half], streams[m], halves[half]]
        return [same(piece, dev) for _, dev, _ in first[half]]

    def slope_of(upward, pre):
        sig = jax.nn.sigmoid(pre)
        return (upward * sig * (1.0 + pre * (1.0 - sig))).astype(BF)

    def q1(k, copies):
        wait_all(copies)
        g[k, core, z2] = plus(g[k, core, z2], rc[k, z2]).astype(BF)
        return [
            remote(g.at[k, core, z2, lo, :], ra.at[k, 0], up),
            remote(g.at[k, core, z2, hi, :], ra.at[k, 1], dn),
        ]

    def q2(k, copies, near):
        near.wait_recv()
        g[k, core, zu, hi, :] = plus(g[k, core, zu, hi, :], rc[k, zu, hi, :]).astype(BF)
        g[k, core, zd, lo, :] = plus(g[k, core, zd, lo, :], rc[k, zd, lo, :]).astype(BF)
        wait_all(copies)
        g[k, core, zu, lo, :] = plus(g[k, core, zu, lo, :], rc[k, zu, lo, :], ra[k, 0]).astype(BF)
        g[k, core, zd, hi, :] = plus(g[k, core, zd, hi, :], rc[k, zd, hi, :], ra[k, 1]).astype(BF)
        return [
            remote(g.at[k, core, zu], rb.at[k, 0], up),
            remote(g.at[k, core, zd], rb.at[k, 1], dn),
        ]

    def fold(value):
        lanes = value.shape[-1]
        value = value.reshape(sub // 8, 8, lanes).sum(0)
        total = value[:, 0:128]
        for i in range(1, lanes // 128):
            total = total + value[:, i * 128 : (i + 1) * 128]
        return total

    def finish(k, copies):
        wait_all(copies)
        value = plus(g[k, core, z], rc[k, z], rb[k, 0], rb[k, 1])
        fin[k] = value
        return fold(value * value)

    def hand_over(kind):
        pex[kind] = fin[2 * other + kind].astype(BF)
        return remote(pex.at[kind], prx.at[kind], pair)

    HALVES = (0, 1)

    def both(f):
        return [f(half) for half in HALVES]

    def project_send(src, k, ph, m):
        sent = []
        for half in HALVES:
            project(src, k, ph, half, m)
            sent.append(rs1(ph, half, m))
        return sent

    def all_rs2(ph, m, sent):
        return both(lambda half: rs2(ph, half, m, sent[half]))

    def all_sp2(ref, m, sent):
        return both(lambda half: sp2(ref, half, m, sent[half]))

    def settle(sent):
        for copies in sent:
            wait_all(copies)

    quarter = sub // 4
    cuts = [pl.ds(i * quarter, quarter) for i in range(4)]
    order = (0, 2, 1, 3)
    k_own = (3 * pipe, 1 + pipe)
    k_got = (3 * other, 1 + other)
    for copy in own_load:
        copy.wait()
    e0 = {i: remote(own.at[pipe, cuts[i], :], w.at[3 * pipe, core, z, cuts[i], :], pair) for i in order}
    e1 = remote(own.at[other], w.at[1 + pipe, core, z], pair)
    ca0 = g1(k_own[0])
    for copy in x_load:
        copy.wait()
    x_here, x_swap = swap_tokens(0, x0)
    ca1 = {}
    for i in order:
        e0[i].wait_recv()
        ca1[i] = g1(k_got[0], cuts[i])
    wait_all(ca0)
    cb0 = g2(k_own[0])
    cc0 = g2c(k_own[0])
    cb1 = []
    for i in order:
        wait_all(ca1[i])
        ahead, to, dev = (zd, up, "u") if i < 2 else (zu, dn, "d")
        cb1.append(same(w.at[k_got[0], core, ahead, cuts[i], :], to))
    cc1 = g2c(k_got[0])
    for copy in cot_load:
        copy.wait()
    cot_here, cot_swap = swap_tokens(1, cot)
    ca2 = g1(k_own[1])
    e1.wait_recv()
    ca3 = g1(k_got[1])
    wait_all(cb0)
    cd0 = g3(k_own[0])
    wait_all(cb1)
    cd1 = g3(k_got[0])
    x_here.wait()
    wait_all(x_swap)
    wait_all(cc0 + cc1)
    wait_all(cd0 + cd1)

    p00 = project_send(x0, 0, 0, 0)
    p01 = project_send(x0, 0, 0, 1)
    cot_here.wait()
    wait_all(cot_swap)
    project(cot, 3, 2, 0, 0)
    project(cot, 3, 2, 1, 0)
    p00 = all_rs2(0, 0, p00)
    wait_all(ca2)
    cb2 = g2(k_own[1])
    cc2 = g2c(k_own[1])
    project(cot, 3, 2, 0, 1)
    p01 = all_rs2(0, 1, p01)

    def open_act(m, sent):
        done = []
        for half in HALVES:
            pre = units(0, half, m, sent[half])
            keep[0, half, slots(m), :] = pre
            put(act.at[0], half, m, jax.nn.silu(pre).astype(BF))
            done.append(sp1(act.at[0], half, m))
        return done

    a00 = open_act(0, p00)
    project(cot, 3, 2, 1, 1)
    a01 = open_act(1, p01)
    a00 = all_sp2(act.at[0], 0, a00)
    a01 = all_sp2(act.at[0], 1, a01)
    p20 = both(lambda half: rs1(2, half, 0))
    p21 = both(lambda half: rs1(2, half, 1))
    wait_all(ca3)
    cb3 = g2(k_got[1])
    cc3 = g2c(k_got[1])
    wait_all(cb2)
    cd2 = g3(k_own[1])
    settle(a00)
    wait_all(cb3)
    cd3 = g3(k_got[1])
    wait_all(cc2 + cc3)
    wait_all(cd2 + cd3)
    widen(x0, act.at[0], 1, x1, 0)
    p10 = project_send(x1, 2, 1, 0)
    settle(a01)
    widen(x0, act.at[0], 1, x1, 1)
    p11 = project_send(x1, 2, 1, 1)
    p20 = all_rs2(2, 0, p20)
    p21 = all_rs2(2, 1, p21)
    p10 = all_rs2(1, 0, p10)
    p11 = all_rs2(1, 1, p11)

    def open_slope(m, sent_up, sent_pre):
        done = []
        for half in HALVES:
            upward = units(2, half, m, sent_up[half])
            pre = units(1, half, m, sent_pre[half])
            put(slope.at[1], half, m, slope_of(upward, pre))
            done.append(sp1(slope.at[1], half, m))
            put(act.at[1], half, m, jax.nn.silu(pre).astype(BF))
        return done

    s10 = open_slope(0, p20, p10)
    s11 = open_slope(1, p21, p11)
    s10 = all_sp2(slope.at[1], 0, s10)
    s11 = all_sp2(slope.at[1], 1, s11)
    a10 = both(lambda half: sp1(act.at[1], half, 0))
    a11 = both(lambda half: sp1(act.at[1], half, 1))
    settle(s10)
    widen(cot, slope.at[1], 2, err1, 0)
    p30 = project_send(err1, 1, 3, 0)
    settle(s11)
    widen(cot, slope.at[1], 2, err1, 1)
    p31 = project_send(err1, 1, 3, 1)
    a10 = all_sp2(act.at[1], 0, a10)
    d2, near2 = weight_grad(x1, slope.at[1], 2)
    p30 = all_rs2(3, 0, p30)
    p31 = all_rs2(3, 1, p31)
    a11 = all_sp2(act.at[1], 1, a11)
    d1, near1 = weight_grad(err1, act.at[0], 1)

    def close_slope(m, sent):
        done = []
        for half in HALVES:
            upward = units(3, half, m, sent[half])
            put(slope.at[0], half, m, slope_of(upward, keep[0, half, slots(m), :]))
            done.append(sp1(slope.at[0], half, m))
        return done

    s00 = close_slope(0, p30)
    s01 = close_slope(1, p31)
    d2 = q2(2, d2, near2)
    s00 = all_sp2(slope.at[0], 0, s00)
    s01 = all_sp2(slope.at[0], 1, s01)
    settle(a10)
    settle(a11)
    d3, near3 = weight_grad(cot, act.at[1], 3)
    d1 = q2(1, d1, near1)
    settle(s00)
    settle(s01)
    d0, near0 = weight_grad(x0, slope.at[0], 0)
    d3 = q2(3, d3, near3)
    squares = finish(2, d2)
    squares = squares + finish(1, d1)
    d0 = q2(0, d0, near0)
    squares = squares + finish(3, d3)
    h1 = hand_over(1)
    turned[0] = fin[2 * pipe + 1].T
    writes = [local(turned.at[0], tot_out.at[:, keep_rows])]
    squares = squares + finish(0, d0)
    nsum[0] = squares
    c1 = [remote(nsum.at[0], n2.at[code], dev) for code, dev in xz]
    h0 = hand_over(0)
    writes.append(local(fin.at[2 * pipe], tot_in.at[keep_rows, :]))
    wait_all(c1)
    total = nsum[0]
    for code in range(1, 16):
        total = total + n2[code]
    nsum[1] = total
    c2 = [remote(nsum.at[1], n1.at[code], dev) for code, dev, _, _ in ycore]
    h1.wait_recv()
    turned[1] = prx[1].astype(F32).T
    writes.append(local(turned.at[1], tot_out.at[:, give_rows]))
    wait_all(c2)
    total = nsum[1]
    for code in range(1, 8):
        total = total + n1[code]
    norm = jnp.sqrt(jnp.sum(total, keepdims=True))
    norm_out[...] = jnp.broadcast_to(norm, norm_out.shape)
    h0.wait_recv()
    late[...] = prx[0].astype(F32)
    writes.append(local(late, tot_in.at[give_rows, :]))
    for copy in started:
        copy.wait_send()
    for copy in writes:
        copy.wait()


def on_device(inputs, w_in, w_out, cotangent):
    micro, tok, cols = inputs.shape
    shard, hid = w_in.shape[1], w_in.shape[2]
    sub = shard // 2
    part_d = cols // 4
    group = micro * tok // 2
    hl = hid // 2
    any_spec = pl.BlockSpec(memory_space=pl.ANY)
    vmem = pl.BlockSpec(memory_space=pltpu.VMEM)
    tokens = pltpu.VMEM((RING, micro, tok // 2, part_d), BF)
    weights = pltpu.VMEM((4, 2, RING, sub, hid), BF)
    layers = pltpu.VMEM((2, RING, group, hid), BF)
    tot_in, tot_out, norm = pl.pallas_call(
        kernel,
        out_shape=(
            jax.ShapeDtypeStruct((shard, hid), F32),
            jax.ShapeDtypeStruct((hid, shard), F32),
            jax.ShapeDtypeStruct((8, 128), F32),
        ),
        in_specs=[any_spec] * 4,
        out_specs=(any_spec, any_spec, vmem),
        scratch_shapes=[
            pltpu.VMEM((2, RING, micro, tok, RING * sub), BF),
            tokens, tokens, tokens, tokens,
            pltpu.VMEM((2, hid, sub), BF),
            pltpu.VMEM((2, sub, hid), BF),
            weights, weights, layers, layers,
            pltpu.VMEM((4, RING, group, hid), BF),
            pltpu.VMEM((4, 2, RING, group, hl), BF),
            pltpu.VMEM((4, 2, RING, group // RING, hl), BF),
            pltpu.VMEM((2, 2, group // RING, hl), F32),
            pltpu.VMEM((4, RING, sub, hid), BF),
            pltpu.VMEM((4, 2, sub // 2, hid), BF),
            pltpu.VMEM((4, 2, sub, hid), BF),
            pltpu.VMEM((4, sub, hid), F32),
            pltpu.VMEM((2, sub, hid), BF),
            pltpu.VMEM((2, sub, hid), BF),
            pltpu.VMEM((sub, hid), F32),
            pltpu.VMEM((2, hid, sub), F32),
            pltpu.VMEM((2, 8, 128), F32),
            pltpu.VMEM((8, 8, 128), F32),
            pltpu.VMEM((16, 8, 128), F32),
            pltpu.SemaphoreType.DMA((48,)),
            pltpu.SemaphoreType.DMA((320,)),
            pltpu.SemaphoreType.DMA((320,)),
        ],
        compiler_params=pltpu.CompilerParams(
            collective_id=0, has_side_effects=True, vmem_limit_bytes=67043328
        ),
    )(inputs, w_in[0], w_out[0], cotangent)
    grad_norm = norm[0, 0]
    factor = jnp.minimum(1.0, CLIP_NORM / grad_norm)
    return (tot_in * factor)[None], (tot_out * factor)[None], grad_norm


def solution(mesh):
    split = Mesh(mesh.devices.reshape(mesh.shape["pipe"], 2, 2, RING, RING), AXES)
    placed = (
        P(None, DP, TENSOR),
        P("pipe", TENSOR_DP, None),
        P("pipe", None, TENSOR_DP),
        P(None, DP, TENSOR),
    )
    return jax.shard_map(
        on_device,
        mesh=split,
        in_specs=placed,
        out_specs=(P("pipe", TENSOR_DP, None), P("pipe", None, TENSOR_DP), P()),
        check_vma=False,
    )
```

```python
import jax
import jax.numpy as jnp
from jax import lax
from jax.experimental import pallas as pl
from jax.experimental.pallas import tpu as pltpu
from jax.sharding import Mesh
from jax.sharding import PartitionSpec as P

CLIP_NORM = 16384.0
AXES = ("pipe", "xhi", "core", "z", "y")
TENSOR = ("xhi", "core")
DP = ("z", "y")
PIPE_TENSOR_DP = ("pipe", "xhi", "core", "z", "y")
TENSOR_DP = ("xhi", "core", "z", "y")
MESH = pl.DeviceIdType.MESH
BF = jnp.bfloat16
F32 = jnp.float32

RING = 4
NT = (((1,), (1,)), ((), ()))
TN = (((0,), (0,)), ((), ()))


def kernel(
    x_hbm, win_hbm, wout_hbm, cot_hbm,
    tot_in, tot_out, norm_out,
    stage, x0, cot, x1, err1, raw, own, w, g, act, slope,
    part, r1, r2, keep,
    rc, ra, rb,
    fin, pex, prx, late, turned, nsum, n1, n2,
    lsem, ssem, rsem,
):
    group, hid = part.shape[2], part.shape[3]
    rows = RING * group
    sub = w.shape[3]
    hl = hid // 2
    hs = sub // 2
    part_d = x0.shape[-1]
    tile = 256
    pipe = lax.axis_index("pipe")
    xhi = lax.axis_index("xhi")
    core = lax.axis_index("core")
    z = lax.axis_index("z")
    y = lax.axis_index("y")
    other = 1 - pipe
    core2 = 1 - core
    xi = xhi * 2 + pipe

    def turn(v, d):
        return lax.rem(v + d, RING)

    started = []
    count = [0]
    lcount = [0]

    class Group:
        def __init__(self, like):
            i = count[0]
            count[0] += 1
            self.sems = {"send_sem": ssem.at[i], "recv_sem": rsem.at[i]}
            self.like = like

        def send(self, src, dst, dev):
            pltpu.make_async_remote_copy(
                src_ref=src, dst_ref=dst, device_id=dev, device_id_type=MESH, **self.sems
            ).start()
            if self not in started:
                self.whole = pltpu.make_async_remote_copy(
                    src_ref=self.like, dst_ref=self.like, device_id=dev, device_id_type=MESH, **self.sems
                )
                started.append(self)
            return self

        def wait_recv(self):
            self.whole.wait_recv()

        def wait_send(self):
            self.whole.wait_send()

    def remote(src, dst, dev):
        return Group(src).send(src, dst, dev)

    def same(ref, dev):
        return remote(ref, ref, dev)

    def group_of(like, items):
        made = Group(like)
        for src, dst, dev in items:
            made.send(src, dst, dev)
        return [made]

    class Local:
        def __init__(self, like):
            self.sem = lsem.at[lcount[0]]
            lcount[0] += 1
            self.whole = pltpu.make_async_copy(like, like, self.sem)

        def start(self, src, dst):
            pltpu.make_async_copy(src, dst, self.sem).start()
            return self

        def wait(self):
            self.whole.wait()

    def local(src, dst):
        return Local(dst).start(src, dst)

    def wait_all(copies):
        for copy in copies:
            copy.wait_recv()

    xpeers = []
    for code in (3, 2, 1):
        p_ = other if code % 2 else pipe
        h_ = 1 - xhi if code // 2 else xhi
        xpeers.append((code, {"pipe": p_, "xhi": h_}, h_ * 2 + p_))
    ypeers = [(d, {"y": turn(y, d)}, turn(y, d)) for d in (2, 1, 3)]
    zpeers = [(d, {"z": turn(z, d)}) for d in (1, 2, 3)]
    up, dn = {"z": turn(z, 1)}, {"z": turn(z, 3)}
    zu, zd, z2 = turn(z, 1), turn(z, 3), turn(z, 2)
    twin = {"core": core2}
    pair = {"pipe": other}
    ycore = [(d * 2, {**dev}, yy, core) for d, dev, yy in ypeers]
    ycore += [(d * 2 + 1, {**dev, "core": core2}, yy, core2) for d, dev, yy in ypeers]
    ycore += [(1, twin, y, core2)]
    xz = [(code, dev) for code, dev, _ in xpeers]
    xz += [(d * 4, dev) for d, dev in zpeers]
    xz += [(d * 4 + code, {**dx, **dz}) for d, dz in zpeers for code, dx, _ in xpeers]

    keep_rows = pl.ds(pl.multiple_of(pipe * sub, sub), sub)
    give_rows = pl.ds(pl.multiple_of(other * sub, sub), sub)
    out_load = [
        local(wout_hbm.at[:, give_rows], raw.at[0]),
        local(wout_hbm.at[:, keep_rows], raw.at[1]),
    ]
    own_load = [
        local(win_hbm.at[give_rows, :], own.at[0]),
        local(win_hbm.at[keep_rows, :], w.at[2 * pipe, core, z]),
    ]

    def fetch(src, n):
        copies = Local(stage.at[n])
        for yy in range(RING):
            for zz in range(RING):
                off = pl.multiple_of((zz * RING + yy) * 2 * sub + pipe * sub, sub)
                copies.start(src.at[:, :, pl.ds(off, sub)], stage.at[n, yy, :, :, pl.ds(zz * sub, sub)])
        return copies

    x_load = fetch(x_hbm, 0)
    cot_load = fetch(cot_hbm, 1)

    barrier = pltpu.get_barrier_semaphore()
    peers = [dev for _, dev, _, _ in ycore] + [dev for _, dev in xz]
    for dev in peers:
        pl.semaphore_signal(barrier, inc=1, device_id=dev, device_id_type=MESH)
    for copy in out_load:
        copy.wait()
    own[1] = raw[0].T
    w[2 * pipe + 1, core, z] = raw[1].T
    pl.semaphore_wait(barrier, len(peers))

    half_tok = x0.shape[2]
    my_cols = pl.ds(pl.multiple_of(core * (part_d // 2), part_d // 2), part_d // 2)

    def swap_tokens(n, dst):
        def piece(yy, cc):
            toks = pl.ds(pl.multiple_of(cc * half_tok, half_tok), half_tok)
            return stage.at[n, yy, :, toks, :]

        landing = dst.at[y, :, :, my_cols]
        return local(piece(y, core), landing), group_of(
            r1.at[n, pl.ds(1, 7)], [(piece(yy, cc), landing, dev) for _, dev, yy, cc in ycore]
        )

    lo, hi = pl.ds(0, hs), pl.ds(hs, hs)

    def g1(k, rows_of=slice(None)):
        ref = w.at[k, core, z, rows_of, :]
        return group_of(w.at[k, core, pl.ds(0, 2), rows_of, :], [(ref, ref, up), (ref, ref, dn)])

    def g2(k):
        a, b = w.at[k, core, zd, lo, :], w.at[k, core, zu, hi, :]
        return group_of(w.at[k, core, z], [(a, a, up), (b, b, dn)])

    def g2c(k):
        refs = [w.at[k, core, at] for at in (z, zu, zd)]
        return group_of(w.at[k, core, pl.ds(0, 3)], [(ref, ref, twin) for ref in refs])

    def g3(k):
        return [same(w.at[k, core, z2], twin)]

    halves = (pl.ds(0, hl), pl.ds(hl, hl))

    mrows = group // 2
    streams = (pl.ds(0, mrows), pl.ds(mrows, mrows))
    srows = RING * mrows

    def project(src, k, ph, half, m):
        @pl.loop(0, hl // tile)
        def _(n):
            cols = pl.ds(pl.multiple_of(half * hl + n * tile, tile), tile)
            left = src[:, m].reshape(srows, part_d)
            right = w[k, :, :, :, cols].reshape(part_d, tile)
            got = jnp.dot(left, right, preferred_element_type=F32)
            part[ph, :, streams[m], cols] = got.astype(BF).reshape(RING, mrows, tile)

    def widen(base, units_ref, k, out, m):
        for cc in range(2):
            @pl.loop(0, 2)
            def _(p):
                cols = pl.ds(pl.multiple_of(cc * RING * sub + p * 2 * sub, tile), 2 * sub)
                left = units_ref[:, streams[m], :].reshape(srows, hid)
                right = w[k, cc, pl.ds(p * 2, 2)].reshape(2 * sub, hid)
                add = lax.dot_general(left, right, NT, preferred_element_type=F32)
                old = base[:, m, :, cols].reshape(srows, 2 * sub).astype(F32)
                out[:, m, :, cols] = (old + add).astype(BF).reshape(RING, mrows, 2 * sub)

    def weight_grad(left_ref, right, k):
        def side(cc, p):
            zz = pl.ds(pl.multiple_of(p * 2, 2), 2)
            cols = pl.ds(pl.multiple_of(cc * RING * sub + p * 2 * sub, tile), 2 * sub)
            left = left_ref[:, :, :, cols].reshape(rows, 2 * sub)
            got = lax.dot_general(left, right[...].reshape(rows, hid), TN, preferred_element_type=F32)
            g[k, cc, zz] = got.astype(BF).reshape(2, sub, hid)

        def across(p):
            zz = pl.ds(pl.multiple_of(p * 2, 2), 2)
            return remote(g.at[k, core2, zz], rc.at[k, zz], twin)

        p_far = z2 // 2
        p_near = 1 - p_far
        side(core2, p_far)
        far = across(p_far)
        side(core2, p_near)
        near = across(p_near)
        side(core, p_far)
        sent = q1(k, [far])
        side(core, p_near)
        return sent, near

    def plus(x, *more):
        total = x.astype(F32)
        for m in more:
            total = total + m.astype(F32)
        return total

    first = (xpeers, ypeers)
    second = (ypeers, xpeers)
    block = (xi, y)
    inner = (y, xi)

    crows = mrows // RING

    def inner_rows(at, m):
        return pl.ds(pl.multiple_of(m * mrows + at * crows, crows), crows)

    def slots(m):
        return pl.ds(m * crows, crows)

    def r1_at(half, slot):
        return half * RING + slot

    def rs1(ph, half, m):
        lanes, r = halves[half], streams[m]
        return group_of(
            r1.at[ph, pl.ds(r1_at(half, 1), 3), r],
            [
                (part.at[ph, at, r, lanes], r1.at[ph, r1_at(half, slot), r], dev)
                for slot, dev, at in first[half]
            ],
        )

    def rs2(ph, half, m, copies):
        wait_all(copies)
        lanes, r = halves[half], streams[m]
        b = block[half]
        part[ph, b, r, lanes] = plus(
            part[ph, b, r, lanes], *[r1[ph, r1_at(half, slot), r] for slot in (1, 2, 3)]
        ).astype(BF)
        return group_of(
            r2.at[ph, half, pl.ds(1, 3), slots(m)],
            [
                (part.at[ph, b, inner_rows(at, m), lanes], r2.at[ph, half, slot, slots(m)], dev)
                for slot, dev, at in second[half]
            ],
        )

    def units(ph, half, m, copies):
        wait_all(copies)
        c = slots(m)
        return plus(
            part[ph, block[half], inner_rows(inner[half], m), halves[half]],
            r2[ph, half, 1, c], r2[ph, half, 2, c], r2[ph, half, 3, c],
        )

    def put(ref, half, m, value):
        ref[block[half], inner_rows(inner[half], m), halves[half]] = value

    def sp1(ref, half, m):
        piece = ref.at[block[half], inner_rows(inner[half], m), halves[half]]
        like = ref.at[block[half], pl.ds(m * mrows, 3 * crows), halves[half]]
        return group_of(like, [(piece, piece, dev) for _, dev, _ in second[half]])

    def sp2(ref, half, m, copies):
        wait_all(copies)
        piece = ref.at[block[half], streams[m], halves[half]]
        like = ref.at[pl.ds(0, 3), streams[m], halves[half]]
        return group_of(like, [(piece, piece, dev) for _, dev, _ in first[half]])

    def slope_of(upward, pre):
        sig = jax.nn.sigmoid(pre)
        return (upward * sig * (1.0 + pre * (1.0 - sig))).astype(BF)

    def q1(k, copies):
        wait_all(copies)
        g[k, core, z2] = plus(g[k, core, z2], rc[k, z2]).astype(BF)
        return group_of(
            ra.at[k],
            [
                (g.at[k, core, z2, lo, :], ra.at[k, 0], up),
                (g.at[k, core, z2, hi, :], ra.at[k, 1], dn),
            ],
        )

    def q2(k, copies, near):
        near.wait_recv()
        g[k, core, zu, hi, :] = plus(g[k, core, zu, hi, :], rc[k, zu, hi, :]).astype(BF)
        g[k, core, zd, lo, :] = plus(g[k, core, zd, lo, :], rc[k, zd, lo, :]).astype(BF)
        wait_all(copies)
        g[k, core, zu, lo, :] = plus(g[k, core, zu, lo, :], rc[k, zu, lo, :], ra[k, 0]).astype(BF)
        g[k, core, zd, hi, :] = plus(g[k, core, zd, hi, :], rc[k, zd, hi, :], ra[k, 1]).astype(BF)
        return group_of(
            rb.at[k], [(g.at[k, core, zu], rb.at[k, 0], up), (g.at[k, core, zd], rb.at[k, 1], dn)]
        )

    def fold(value):
        lanes = value.shape[-1]
        value = value.reshape(sub // 8, 8, lanes).sum(0)
        total = value[:, 0:128]
        for i in range(1, lanes // 128):
            total = total + value[:, i * 128 : (i + 1) * 128]
        return total

    def finish(k, copies):
        wait_all(copies)
        value = plus(g[k, core, z], rc[k, z], rb[k, 0], rb[k, 1])
        fin[k] = value
        return fold(value * value)

    def hand_over(kind):
        pex[kind] = fin[2 * other + kind].astype(BF)
        return remote(pex.at[kind], prx.at[kind], pair)

    HALVES = (0, 1)

    def both(f):
        return [f(half) for half in HALVES]

    def project_send(src, k, ph, m):
        sent = []
        for half in HALVES:
            project(src, k, ph, half, m)
            sent.append(rs1(ph, half, m))
        return sent

    def all_rs2(ph, m, sent):
        return both(lambda half: rs2(ph, half, m, sent[half]))

    def all_sp2(ref, m, sent):
        return both(lambda half: sp2(ref, half, m, sent[half]))

    def settle(sent):
        for copies in sent:
            wait_all(copies)

    quarter = sub // 4
    cuts = [pl.ds(i * quarter, quarter) for i in range(4)]
    order = (0, 2, 1, 3)
    k_own = (3 * pipe, 1 + pipe)
    k_got = (3 * other, 1 + other)
    for copy in own_load:
        copy.wait()
    e0 = {i: remote(own.at[pipe, cuts[i], :], w.at[3 * pipe, core, z, cuts[i], :], pair) for i in order}
    e1 = remote(own.at[other], w.at[1 + pipe, core, z], pair)
    ca0 = g1(k_own[0])
    x_load.wait()
    x_here, x_swap = swap_tokens(0, x0)
    cot_load.wait()
    cot_here, cot_swap = swap_tokens(1, cot)
    ca1 = {}
    for i in order:
        e0[i].wait_recv()
        ca1[i] = g1(k_got[0], cuts[i])
    wait_all(ca0)
    cb0 = g2(k_own[0])
    cc0 = g2c(k_own[0])
    cb1 = Group(w.at[k_got[0], core, z])
    for i in order:
        wait_all(ca1[i])
        ahead, to = (zd, up) if i < 2 else (zu, dn)
        ref = w.at[k_got[0], core, ahead, cuts[i], :]
        cb1.send(ref, ref, to)
    cc1 = g2c(k_got[0])
    ca2 = g1(k_own[1])
    e1.wait_recv()
    ca3 = g1(k_got[1])
    wait_all(cb0)
    cd0 = g3(k_own[0])
    cb1.wait_recv()
    cd1 = g3(k_got[0])
    x_here.wait()
    wait_all(x_swap)
    wait_all(cc0 + cc1)
    wait_all(cd0 + cd1)

    p00 = project_send(x0, 0, 0, 0)
    p01 = project_send(x0, 0, 0, 1)
    wait_all(ca2)
    cb2 = g2(k_own[1])
    cc2 = g2c(k_own[1])
    cot_here.wait()
    wait_all(cot_swap)
    for m in (0, 1):
        for half in HALVES:
            project(cot, 3, 2, half, m)
    p00 = all_rs2(0, 0, p00)
    wait_all(ca3)
    cb3 = g2(k_got[1])
    cc3 = g2c(k_got[1])
    p01 = all_rs2(0, 1, p01)

    def open_act(m, sent):
        done = []
        for half in HALVES:
            pre = units(0, half, m, sent[half])
            keep[0, half, slots(m), :] = pre
            put(act.at[0], half, m, jax.nn.silu(pre).astype(BF))
            done.append(sp1(act.at[0], half, m))
        return done

    a00 = open_act(0, p00)
    a01 = open_act(1, p01)
    a00 = all_sp2(act.at[0], 0, a00)
    a01 = all_sp2(act.at[0], 1, a01)
    p20 = both(lambda half: rs1(2, half, 0))
    p21 = both(lambda half: rs1(2, half, 1))
    wait_all(cb2)
    cd2 = g3(k_own[1])
    wait_all(cb3)
    cd3 = g3(k_got[1])
    wait_all(cc2 + cc3)
    wait_all(cd2 + cd3)
    settle(a00)
    widen(x0, act.at[0], 1, x1, 0)
    p10 = project_send(x1, 2, 1, 0)
    settle(a01)
    widen(x0, act.at[0], 1, x1, 1)
    p11 = project_send(x1, 2, 1, 1)
    p20 = all_rs2(2, 0, p20)
    p21 = all_rs2(2, 1, p21)
    p10 = all_rs2(1, 0, p10)
    p11 = all_rs2(1, 1, p11)

    def open_slope(m, sent_up, sent_pre):
        done = []
        for half in HALVES:
            upward = units(2, half, m, sent_up[half])
            pre = units(1, half, m, sent_pre[half])
            put(slope.at[1], half, m, slope_of(upward, pre))
            done.append(sp1(slope.at[1], half, m))
            put(act.at[1], half, m, jax.nn.silu(pre).astype(BF))
        return done

    s10 = open_slope(0, p20, p10)
    s11 = open_slope(1, p21, p11)
    s10 = all_sp2(slope.at[1], 0, s10)
    s11 = all_sp2(slope.at[1], 1, s11)
    a10 = both(lambda half: sp1(act.at[1], half, 0))
    a11 = both(lambda half: sp1(act.at[1], half, 1))
    settle(s10)
    widen(cot, slope.at[1], 2, err1, 0)
    p30 = project_send(err1, 1, 3, 0)
    settle(s11)
    widen(cot, slope.at[1], 2, err1, 1)
    p31 = project_send(err1, 1, 3, 1)
    a10 = all_sp2(act.at[1], 0, a10)
    d2, near2 = weight_grad(x1, slope.at[1], 2)
    p30 = all_rs2(3, 0, p30)
    p31 = all_rs2(3, 1, p31)
    a11 = all_sp2(act.at[1], 1, a11)
    d1, near1 = weight_grad(err1, act.at[0], 1)
    d2 = q2(2, d2, near2)

    def close_slope(m, sent):
        done = []
        for half in HALVES:
            upward = units(3, half, m, sent[half])
            put(slope.at[0], half, m, slope_of(upward, keep[0, half, slots(m), :]))
            done.append(sp1(slope.at[0], half, m))
        return done

    s00 = close_slope(0, p30)
    s01 = close_slope(1, p31)
    s00 = all_sp2(slope.at[0], 0, s00)
    s01 = all_sp2(slope.at[0], 1, s01)
    settle(a10)
    settle(a11)
    d3, near3 = weight_grad(cot, act.at[1], 3)
    d1 = q2(1, d1, near1)
    settle(s00)
    settle(s01)
    d0, near0 = weight_grad(x0, slope.at[0], 0)
    d3 = q2(3, d3, near3)
    squares = finish(2, d2)
    squares = squares + finish(1, d1)
    d0 = q2(0, d0, near0)
    squares = squares + finish(3, d3)
    h1 = hand_over(1)
    turned[0] = fin[2 * pipe + 1].T
    writes = [local(turned.at[0], tot_out.at[:, keep_rows])]
    squares = squares + finish(0, d0)
    nsum[0] = squares
    c1 = group_of(n2.at[pl.ds(1, 15)], [(nsum.at[0], n2.at[code], dev) for code, dev in xz])
    h0 = hand_over(0)
    writes.append(local(fin.at[2 * pipe], tot_in.at[keep_rows, :]))
    wait_all(c1)
    total = nsum[0]
    for code in range(1, 16):
        total = total + n2[code]
    nsum[1] = total
    c2 = group_of(n1.at[pl.ds(1, 7)], [(nsum.at[1], n1.at[code], dev) for code, dev, _, _ in ycore])
    h1.wait_recv()
    turned[1] = prx[1].astype(F32).T
    writes.append(local(turned.at[1], tot_out.at[:, give_rows]))
    wait_all(c2)
    total = nsum[1]
    for code in range(1, 8):
        total = total + n1[code]
    norm = jnp.sqrt(jnp.sum(total, keepdims=True))
    norm_out[...] = norm
    h0.wait_recv()
    late[...] = prx[0].astype(F32)
    writes.append(local(late, tot_in.at[give_rows, :]))
    for copy in started:
        copy.wait_send()
    for copy in writes:
        copy.wait()


def on_device(inputs, w_in, w_out, cotangent):
    micro, tok, cols = inputs.shape
    shard, hid = w_in.shape[1], w_in.shape[2]
    sub = shard // 2
    part_d = cols // 4
    group = micro * tok // 2
    hl = hid // 2
    any_spec = pl.BlockSpec(memory_space=pl.ANY)
    vmem = pl.BlockSpec(memory_space=pltpu.VMEM)
    tokens = pltpu.VMEM((RING, micro, tok // 2, part_d), BF)
    weights = pltpu.VMEM((4, 2, RING, sub, hid), BF)
    layers = pltpu.VMEM((2, RING, group, hid), BF)
    tot_in, tot_out, norm = pl.pallas_call(
        kernel,
        out_shape=(
            jax.ShapeDtypeStruct((shard, hid), F32),
            jax.ShapeDtypeStruct((hid, shard), F32),
            jax.ShapeDtypeStruct((1, 1), F32),
        ),
        in_specs=[any_spec] * 4,
        out_specs=(any_spec, any_spec, vmem),
        scratch_shapes=[
            pltpu.VMEM((2, RING, micro, tok, RING * sub), BF),
            tokens, tokens, tokens, tokens,
            pltpu.VMEM((2, hid, sub), BF),
            pltpu.VMEM((2, sub, hid), BF),
            weights, weights, layers, layers,
            pltpu.VMEM((4, RING, group, hid), BF),
            pltpu.VMEM((4, 2 * RING, group, hl), BF),
            pltpu.VMEM((4, 2, RING, group // RING, hl), BF),
            pltpu.VMEM((2, 2, group // RING, hl), F32),
            pltpu.VMEM((4, RING, sub, hid), BF),
            pltpu.VMEM((4, 2, sub // 2, hid), BF),
            pltpu.VMEM((4, 2, sub, hid), BF),
            pltpu.VMEM((4, sub, hid), F32),
            pltpu.VMEM((2, sub, hid), BF),
            pltpu.VMEM((2, sub, hid), BF),
            pltpu.VMEM((sub, hid), F32),
            pltpu.VMEM((2, hid, sub), F32),
            pltpu.VMEM((2, 8, 128), F32),
            pltpu.VMEM((8, 8, 128), F32),
            pltpu.VMEM((16, 8, 128), F32),
            pltpu.SemaphoreType.DMA((12,)),
            pltpu.SemaphoreType.DMA((110,)),
            pltpu.SemaphoreType.DMA((110,)),
        ],
        compiler_params=pltpu.CompilerParams(
            collective_id=0, has_side_effects=True, vmem_limit_bytes=67043328
        ),
    )(inputs, w_in[0], w_out[0], cotangent)
    grad_norm = norm[0, 0]
    factor = jnp.minimum(1.0, CLIP_NORM / grad_norm)
    return (tot_in * factor)[None], (tot_out * factor)[None], grad_norm


def solution(mesh):
    split = Mesh(mesh.devices.reshape(mesh.shape["pipe"], 2, 2, RING, RING), AXES)
    placed = (
        P(None, DP, TENSOR),
        P("pipe", TENSOR_DP, None),
        P("pipe", None, TENSOR_DP),
        P(None, DP, TENSOR),
    )
    return jax.shard_map(
        on_device,
        mesh=split,
        in_specs=placed,
        out_specs=(P("pipe", TENSOR_DP, None), P("pipe", None, TENSOR_DP), P()),
        check_vma=False,
    )
```

```python
import jax
import jax.numpy as jnp
from jax import lax
from jax.experimental import pallas as pl
from jax.experimental.pallas import tpu as pltpu
from jax.sharding import Mesh
from jax.sharding import PartitionSpec as P

CLIP_NORM = 16384.0
AXES = ("pipe", "xhi", "core", "z", "y")
TENSOR = ("xhi", "core")
DP = ("z", "y")
PIPE_TENSOR_DP = ("pipe", "xhi", "core", "z", "y")
TENSOR_DP = ("xhi", "core", "z", "y")
MESH = pl.DeviceIdType.MESH
BF = jnp.bfloat16
F32 = jnp.float32

RING = 4
NT = (((1,), (1,)), ((), ()))
TN = (((0,), (0,)), ((), ()))


def kernel(
    x_hbm, win_hbm, wout_hbm, cot_hbm,
    tot_in, tot_out, norm_out,
    stage, x0, cot, x1, err1, raw, own, w, g, act, slope,
    part, r1, rx, r2, keep,
    rc, ra, rb,
    fin, pex, prx, late, turned, nsum, n1, n2,
    lsem, ssem, rsem,
):
    group, hid = part.shape[2], part.shape[3]
    rows = RING * group
    sub = w.shape[3]
    hl = hid // 2
    hs = sub // 2
    part_d = x0.shape[-1]
    tile = 256
    pipe = lax.axis_index("pipe")
    xhi = lax.axis_index("xhi")
    core = lax.axis_index("core")
    z = lax.axis_index("z")
    y = lax.axis_index("y")
    other = 1 - pipe
    core2 = 1 - core
    xi = xhi * 2 + pipe

    def turn(v, d):
        return lax.rem(v + d, RING)

    started = []
    count = [0]
    lcount = [0]

    class Group:
        def __init__(self, like):
            i = count[0]
            count[0] += 1
            self.sems = {"send_sem": ssem.at[i], "recv_sem": rsem.at[i]}
            self.like = like

        def send(self, src, dst, dev):
            pltpu.make_async_remote_copy(
                src_ref=src, dst_ref=dst, device_id=dev, device_id_type=MESH, **self.sems
            ).start()
            if self not in started:
                self.whole = pltpu.make_async_remote_copy(
                    src_ref=self.like, dst_ref=self.like, device_id=dev, device_id_type=MESH, **self.sems
                )
                started.append(self)
            return self

        def wait_recv(self):
            self.whole.wait_recv()

        def wait_send(self):
            self.whole.wait_send()

    def remote(src, dst, dev):
        return Group(src).send(src, dst, dev)

    def same(ref, dev):
        return remote(ref, ref, dev)

    def group_of(like, items):
        made = Group(like)
        for src, dst, dev in items:
            made.send(src, dst, dev)
        return [made]

    class Local:
        def __init__(self, like):
            self.sem = lsem.at[lcount[0]]
            lcount[0] += 1
            self.whole = pltpu.make_async_copy(like, like, self.sem)

        def start(self, src, dst):
            pltpu.make_async_copy(src, dst, self.sem).start()
            return self

        def wait(self):
            self.whole.wait()

    def local(src, dst):
        return Local(dst).start(src, dst)

    def wait_all(copies):
        for copy in copies:
            copy.wait_recv()

    xpeers = []
    for code in (3, 2, 1):
        p_ = other if code % 2 else pipe
        h_ = 1 - xhi if code // 2 else xhi
        xpeers.append((code, {"pipe": p_, "xhi": h_}, h_ * 2 + p_))
    ypeers = [(d, {"y": turn(y, d)}, turn(y, d)) for d in (2, 1, 3)]
    zpeers = [(d, {"z": turn(z, d)}) for d in (1, 2, 3)]
    up, dn = {"z": turn(z, 1)}, {"z": turn(z, 3)}
    zu, zd, z2 = turn(z, 1), turn(z, 3), turn(z, 2)
    twin = {"core": core2}
    pair = {"pipe": other}
    ycore = [(d * 2, {**dev}, yy, core) for d, dev, yy in ypeers]
    ycore += [(d * 2 + 1, {**dev, "core": core2}, yy, core2) for d, dev, yy in ypeers]
    ycore += [(1, twin, y, core2)]
    xz = [(code, dev) for code, dev, _ in xpeers]
    xz += [(d * 4, dev) for d, dev in zpeers]
    xz += [(d * 4 + code, {**dx, **dz}) for d, dz in zpeers for code, dx, _ in xpeers]

    keep_rows = pl.ds(pl.multiple_of(pipe * sub, sub), sub)
    give_rows = pl.ds(pl.multiple_of(other * sub, sub), sub)
    out_load = [
        local(wout_hbm.at[:, give_rows], raw.at[0]),
        local(wout_hbm.at[:, keep_rows], raw.at[1]),
    ]
    own_load = [
        local(win_hbm.at[give_rows, :], own.at[0]),
        local(win_hbm.at[keep_rows, :], w.at[2 * pipe, core, z]),
    ]

    def fetch(src, n):
        copies = Local(stage.at[n])
        for yy in range(RING):
            for zz in range(RING):
                off = pl.multiple_of((zz * RING + yy) * 2 * sub + pipe * sub, sub)
                copies.start(src.at[:, :, pl.ds(off, sub)], stage.at[n, yy, :, :, pl.ds(zz * sub, sub)])
        return copies

    x_load = fetch(x_hbm, 0)
    cot_load = fetch(cot_hbm, 1)

    barrier = pltpu.get_barrier_semaphore()
    peers = [dev for _, dev, _, _ in ycore] + [dev for _, dev in xz]
    for dev in peers:
        pl.semaphore_signal(barrier, inc=1, device_id=dev, device_id_type=MESH)
    for copy in out_load:
        copy.wait()
    own[1] = raw[0].T
    w[2 * pipe + 1, core, z] = raw[1].T
    pl.semaphore_wait(barrier, len(peers))

    half_tok = x0.shape[2]
    my_cols = pl.ds(pl.multiple_of(core * (part_d // 2), part_d // 2), part_d // 2)

    def swap_tokens(n, dst):
        def piece(yy, cc):
            toks = pl.ds(pl.multiple_of(cc * half_tok, half_tok), half_tok)
            return stage.at[n, yy, :, toks, :]

        landing = dst.at[y, :, :, my_cols]
        return local(piece(y, core), landing), group_of(
            r1.at[n, pl.ds(1, 7)], [(piece(yy, cc), landing, dev) for _, dev, yy, cc in ycore]
        )

    lo, hi = pl.ds(0, hs), pl.ds(hs, hs)

    def g1(k, rows_of=slice(None)):
        ref = w.at[k, core, z, rows_of, :]
        return group_of(w.at[k, core, pl.ds(0, 2), rows_of, :], [(ref, ref, up), (ref, ref, dn)])

    def g2(k):
        a, b = w.at[k, core, zd, lo, :], w.at[k, core, zu, hi, :]
        return group_of(w.at[k, core, z], [(a, a, up), (b, b, dn)])

    def g2c(k):
        refs = [w.at[k, core, at] for at in (z, zu, zd)]
        return group_of(w.at[k, core, pl.ds(0, 3)], [(ref, ref, twin) for ref in refs])

    def g3(k):
        return [same(w.at[k, core, z2], twin)]

    halves = (pl.ds(0, hl), pl.ds(hl, hl))

    mrows = group // 2
    streams = (pl.ds(0, mrows), pl.ds(mrows, mrows))
    srows = RING * mrows

    def project(src, k, ph, half, m):
        @pl.loop(0, hl // tile)
        def _(n):
            cols = pl.ds(pl.multiple_of(half * hl + n * tile, tile), tile)
            left = src[:, m].reshape(srows, part_d)
            right = w[k, :, :, :, cols].reshape(part_d, tile)
            got = jnp.dot(left, right, preferred_element_type=F32)
            part[ph, :, streams[m], cols] = got.astype(BF).reshape(RING, mrows, tile)

    def widen(base, units_ref, k, out, m):
        for cc in range(2):
            @pl.loop(0, 2)
            def _(p):
                cols = pl.ds(pl.multiple_of(cc * RING * sub + p * 2 * sub, tile), 2 * sub)
                left = units_ref[:, streams[m], :].reshape(srows, hid)
                right = w[k, cc, pl.ds(p * 2, 2)].reshape(2 * sub, hid)
                add = lax.dot_general(left, right, NT, preferred_element_type=F32)
                old = base[:, m, :, cols].reshape(srows, 2 * sub).astype(F32)
                out[:, m, :, cols] = (old + add).astype(BF).reshape(RING, mrows, 2 * sub)

    def weight_grad(left_ref, right, k):
        def side(cc, p):
            zz = pl.ds(pl.multiple_of(p * 2, 2), 2)
            cols = pl.ds(pl.multiple_of(cc * RING * sub + p * 2 * sub, tile), 2 * sub)
            left = left_ref[:, :, :, cols].reshape(rows, 2 * sub)
            got = lax.dot_general(left, right[...].reshape(rows, hid), TN, preferred_element_type=F32)
            g[k, cc, zz] = got.astype(BF).reshape(2, sub, hid)

        def across(p):
            zz = pl.ds(pl.multiple_of(p * 2, 2), 2)
            return remote(g.at[k, core2, zz], rc.at[k, zz], twin)

        p_far = z2 // 2
        p_near = 1 - p_far
        side(core2, p_far)
        far = across(p_far)
        side(core2, p_near)
        near = across(p_near)
        side(core, p_far)
        side(core, p_near)
        return q1(k, [far]), near

    def plus(x, *more):
        total = x.astype(F32)
        for m in more:
            total = total + m.astype(F32)
        return total

    first = (xpeers, ypeers)
    second = (ypeers, xpeers)
    block = (xi, y)
    inner = (y, xi)

    crows = mrows // RING

    def inner_rows(at, m):
        return pl.ds(pl.multiple_of(m * mrows + at * crows, crows), crows)

    def slots(m):
        return pl.ds(m * crows, crows)

    def r1_at(half, slot):
        return half * RING + slot

    def rs1(ph, half, m):
        lanes, r = halves[half], streams[m]
        return group_of(
            r1.at[ph, pl.ds(r1_at(half, 1), 3), r],
            [
                (part.at[ph, at, r, lanes], r1.at[ph, r1_at(half, slot), r], dev)
                for slot, dev, at in first[half]
            ],
        )

    def rs2(ph, half, m, copies):
        wait_all(copies)
        lanes, r = halves[half], streams[m]
        b = block[half]
        part[ph, b, r, lanes] = plus(
            part[ph, b, r, lanes], *[r1[ph, r1_at(half, slot), r] for slot in (1, 2, 3)]
        ).astype(BF)
        return group_of(
            r2.at[ph, half, pl.ds(1, 3), slots(m)],
            [
                (part.at[ph, b, inner_rows(at, m), lanes], r2.at[ph, half, slot, slots(m)], dev)
                for slot, dev, at in second[half]
            ],
        )

    def rs1_turned(ph, m):
        return group_of(
            rx.at[pl.ds(1, 3)],
            [(part.at[ph, :, inner_rows(at, m), halves[1]], rx.at[slot], dev) for slot, dev, at in xpeers],
        )

    def rs2_turned(ph, m, copies):
        wait_all(copies)
        mid = inner_rows(xi, m)
        part[ph, :, mid, halves[1]] = plus(part[ph, :, mid, halves[1]], rx[1], rx[2], rx[3]).astype(BF)
        return group_of(
            r2.at[ph, 1, pl.ds(1, 3), slots(m)],
            [(part.at[ph, at, mid, halves[1]], r2.at[ph, 1, slot, slots(m)], dev) for slot, dev, at in ypeers],
        )

    def units(ph, half, m, copies):
        wait_all(copies)
        c = slots(m)
        return plus(
            part[ph, block[half], inner_rows(inner[half], m), halves[half]],
            r2[ph, half, 1, c], r2[ph, half, 2, c], r2[ph, half, 3, c],
        )

    def put(ref, half, m, value):
        ref[block[half], inner_rows(inner[half], m), halves[half]] = value

    def sp1(ref, half, m):
        piece = ref.at[block[half], inner_rows(inner[half], m), halves[half]]
        like = ref.at[block[half], pl.ds(m * mrows, 3 * crows), halves[half]]
        return group_of(like, [(piece, piece, dev) for _, dev, _ in second[half]])

    def sp2(ref, half, m, copies):
        wait_all(copies)
        piece = ref.at[block[half], streams[m], halves[half]]
        like = ref.at[pl.ds(0, 3), streams[m], halves[half]]
        return group_of(like, [(piece, piece, dev) for _, dev, _ in first[half]])

    def slope_of(upward, pre):
        sig = jax.nn.sigmoid(pre)
        return (upward * sig * (1.0 + pre * (1.0 - sig))).astype(BF)

    def q1(k, copies):
        wait_all(copies)
        g[k, core, z2] = plus(g[k, core, z2], rc[k, z2]).astype(BF)
        return group_of(
            ra.at[k],
            [
                (g.at[k, core, z2, lo, :], ra.at[k, 0], up),
                (g.at[k, core, z2, hi, :], ra.at[k, 1], dn),
            ],
        )

    def q2(k, copies, near):
        near.wait_recv()
        g[k, core, zu, hi, :] = plus(g[k, core, zu, hi, :], rc[k, zu, hi, :]).astype(BF)
        g[k, core, zd, lo, :] = plus(g[k, core, zd, lo, :], rc[k, zd, lo, :]).astype(BF)
        wait_all(copies)
        g[k, core, zu, lo, :] = plus(g[k, core, zu, lo, :], rc[k, zu, lo, :], ra[k, 0]).astype(BF)
        g[k, core, zd, hi, :] = plus(g[k, core, zd, hi, :], rc[k, zd, hi, :], ra[k, 1]).astype(BF)
        return group_of(
            rb.at[k], [(g.at[k, core, zu], rb.at[k, 0], up), (g.at[k, core, zd], rb.at[k, 1], dn)]
        )

    def fold(value):
        lanes = value.shape[-1]
        value = value.reshape(sub // 8, 8, lanes).sum(0)
        total = value[:, 0:128]
        for i in range(1, lanes // 128):
            total = total + value[:, i * 128 : (i + 1) * 128]
        return total

    def finish(k, copies):
        wait_all(copies)
        value = plus(g[k, core, z], rc[k, z], rb[k, 0], rb[k, 1])
        fin[k] = value
        return fold(value * value)

    def hand_over(kind):
        pex[kind] = fin[2 * other + kind].astype(BF)
        return remote(pex.at[kind], prx.at[kind], pair)

    HALVES = (0, 1)

    def both(f):
        return [f(half) for half in HALVES]

    def project_send(src, k, ph, m):
        sent = []
        for half in HALVES:
            project(src, k, ph, half, m)
            sent.append(rs1(ph, half, m))
        return sent

    def all_rs2(ph, m, sent):
        return both(lambda half: rs2(ph, half, m, sent[half]))

    def all_sp2(ref, m, sent):
        return both(lambda half: sp2(ref, half, m, sent[half]))

    def settle(sent):
        for copies in sent:
            wait_all(copies)

    quarter = sub // 4
    cuts = [pl.ds(i * quarter, quarter) for i in range(4)]
    order = (0, 2, 1, 3)
    def open_act(m, sent):
        done = []
        for half in HALVES:
            pre = units(0, half, m, sent[half])
            keep[0, half, slots(m), :] = pre
            put(act.at[0], half, m, jax.nn.silu(pre).astype(BF))
            done.append(sp1(act.at[0], half, m))
        return done

    own1, got1 = 1 + pipe, 1 + other
    for copy in own_load:
        copy.wait()
    e0 = {i: remote(own.at[pipe, cuts[i], :], w.at[3 * pipe, core, z, cuts[i], :], pair) for i in order}
    e1 = remote(own.at[other], w.at[own1, core, z], pair)
    x_load.wait()
    x_here, x_swap = swap_tokens(0, x0)
    ca_own1 = g1(own1, lo)
    cot_load.wait()
    cot_here, cot_swap = swap_tokens(1, cot)
    ca0 = {}
    for i in order:
        e0[i].wait_recv()
        ca0[i] = g1(0, cuts[i])
    cb0 = Group(w.at[0, core, z])
    for i in order:
        wait_all(ca0[i])
        ahead, to = (zd, up) if i < 2 else (zu, dn)
        ref = w.at[0, core, ahead, cuts[i], :]
        cb0.send(ref, ref, to)
    cc0 = g2c(0)
    ca3 = g1(3)
    ca_own1 += g1(own1, hi)
    e1.wait_recv()
    ca_got1 = g1(got1)
    cb0.wait_recv()
    cd0 = g3(0)
    x_here.wait()
    wait_all(x_swap)
    wait_all(cc0)
    wait_all(cd0)

    project(x0, 0, 0, 0, 0)
    p00a = rs1(0, 0, 0)
    project(x0, 0, 0, 1, 0)
    p00b = rs1_turned(0, 0)
    p01 = project_send(x0, 0, 0, 1)
    wait_all(ca3)
    cb3 = g2(3)
    cc3 = g2c(3)
    wait_all(ca_own1)
    cb_own1 = g2(own1)
    cc_own1 = g2c(own1)
    p00 = [rs2(0, 0, 0, p00a), rs2_turned(0, 0, p00b)]
    p01 = all_rs2(0, 1, p01)
    a00 = open_act(0, p00)
    wait_all(ca_got1)
    cb_got1 = g2(got1)
    cc_got1 = g2c(got1)
    a01 = open_act(1, p01)
    a00 = all_sp2(act.at[0], 0, a00)
    wait_all(cb3)
    cd3 = g3(3)
    a01 = all_sp2(act.at[0], 1, a01)
    cot_here.wait()
    wait_all(cot_swap)
    wait_all(cc3)
    wait_all(cd3)
    p20 = project_send(cot, 3, 2, 0)
    wait_all(cb_own1)
    cd_own1 = g3(own1)
    project(cot, 3, 2, 0, 1)
    project(cot, 3, 2, 1, 1)
    wait_all(cb_got1)
    cd_got1 = g3(got1)
    settle(a00)
    wait_all(cc_own1 + cc_got1)
    wait_all(cd_own1 + cd_got1)
    widen(x0, act.at[0], 1, x1, 0)
    p10 = project_send(x1, 2, 1, 0)
    p21 = both(lambda half: rs1(2, half, 1))
    settle(a01)
    widen(x0, act.at[0], 1, x1, 1)
    p11 = project_send(x1, 2, 1, 1)
    p20 = all_rs2(2, 0, p20)
    p10 = all_rs2(1, 0, p10)
    p21 = all_rs2(2, 1, p21)
    def open_slope(m, sent_up, sent_pre):
        done = []
        for half in HALVES:
            upward = units(2, half, m, sent_up[half])
            pre = units(1, half, m, sent_pre[half])
            put(slope.at[1], half, m, slope_of(upward, pre))
            done.append(sp1(slope.at[1], half, m))
            put(act.at[1], half, m, jax.nn.silu(pre).astype(BF))
        return done

    p11 = all_rs2(1, 1, p11)
    s10 = open_slope(0, p20, p10)
    s11 = open_slope(1, p21, p11)
    s10 = all_sp2(slope.at[1], 0, s10)
    s11 = all_sp2(slope.at[1], 1, s11)
    a10 = both(lambda half: sp1(act.at[1], half, 0))
    a11 = both(lambda half: sp1(act.at[1], half, 1))
    settle(s10)
    widen(cot, slope.at[1], 2, err1, 0)
    p30 = project_send(err1, 1, 3, 0)
    settle(s11)
    d2, near2 = weight_grad(x1, slope.at[1], 2)
    a10 = all_sp2(act.at[1], 0, a10)
    widen(cot, slope.at[1], 2, err1, 1)
    p31 = project_send(err1, 1, 3, 1)
    p30 = all_rs2(3, 0, p30)
    d1, near1 = weight_grad(err1, act.at[0], 1)
    d2 = q2(2, d2, near2)
    def close_slope(m, sent):
        done = []
        for half in HALVES:
            upward = units(3, half, m, sent[half])
            put(slope.at[0], half, m, slope_of(upward, keep[0, half, slots(m), :]))
            done.append(sp1(slope.at[0], half, m))
        return done

    s00 = close_slope(0, p30)
    p31 = all_rs2(3, 1, p31)
    a11 = all_sp2(act.at[1], 1, a11)
    s00 = all_sp2(slope.at[0], 0, s00)
    s01 = close_slope(1, p31)
    d1 = q2(1, d1, near1)
    s01 = all_sp2(slope.at[0], 1, s01)
    settle(a10)
    settle(a11)
    d3, near3 = weight_grad(cot, act.at[1], 3)
    squares = finish(2, d2)
    settle(s00)
    settle(s01)
    d0, near0 = weight_grad(x0, slope.at[0], 0)
    d3 = q2(3, d3, near3)
    squares = squares + finish(1, d1)
    d0 = q2(0, d0, near0)
    squares = squares + finish(3, d3)
    h1 = hand_over(1)
    turned[0] = fin[2 * pipe + 1].T
    writes = [local(turned.at[0], tot_out.at[:, keep_rows])]
    squares = squares + finish(0, d0)
    nsum[0] = squares
    c1 = group_of(n2.at[pl.ds(1, 15)], [(nsum.at[0], n2.at[code], dev) for code, dev in xz])
    h0 = hand_over(0)
    writes.append(local(fin.at[2 * pipe], tot_in.at[keep_rows, :]))
    wait_all(c1)
    total = nsum[0]
    for code in range(1, 16):
        total = total + n2[code]
    nsum[1] = total
    c2 = group_of(n1.at[pl.ds(1, 7)], [(nsum.at[1], n1.at[code], dev) for code, dev, _, _ in ycore])
    h1.wait_recv()
    turned[1] = prx[1].astype(F32).T
    writes.append(local(turned.at[1], tot_out.at[:, give_rows]))
    wait_all(c2)
    total = nsum[1]
    for code in range(1, 8):
        total = total + n1[code]
    norm = jnp.sqrt(jnp.sum(total, keepdims=True))
    norm_out[...] = norm
    h0.wait_recv()
    late[...] = prx[0].astype(F32)
    writes.append(local(late, tot_in.at[give_rows, :]))
    for copy in started:
        copy.wait_send()
    for copy in writes:
        copy.wait()


def clip(norm_ref, tot_in, tot_out, upd_in, upd_out):
    factor = jnp.minimum(1.0, CLIP_NORM / norm_ref[...])
    upd_in[...] = tot_in[...] * factor
    upd_out[...] = tot_out[...] * factor


def on_device(inputs, w_in, w_out, cotangent):
    micro, tok, cols = inputs.shape
    shard, hid = w_in.shape[1], w_in.shape[2]
    sub = shard // 2
    part_d = cols // 4
    group = micro * tok // 2
    hl = hid // 2
    any_spec = pl.BlockSpec(memory_space=pl.ANY)
    vmem = pl.BlockSpec(memory_space=pltpu.VMEM)
    tokens = pltpu.VMEM((RING, micro, tok // 2, part_d), BF)
    weights = pltpu.VMEM((4, 2, RING, sub, hid), BF)
    layers = pltpu.VMEM((2, RING, group, hid), BF)
    tot_in, tot_out, norm = pl.pallas_call(
        kernel,
        out_shape=(
            jax.ShapeDtypeStruct((shard, hid), F32),
            jax.ShapeDtypeStruct((hid, shard), F32),
            jax.ShapeDtypeStruct((1, 1), F32),
        ),
        in_specs=[any_spec] * 4,
        out_specs=(any_spec, any_spec, vmem),
        scratch_shapes=[
            pltpu.VMEM((2, RING, micro, tok, RING * sub), BF),
            tokens, tokens, tokens, tokens,
            pltpu.VMEM((2, hid, sub), BF),
            pltpu.VMEM((2, sub, hid), BF),
            weights, weights, layers, layers,
            pltpu.VMEM((4, RING, group, hid), BF),
            pltpu.VMEM((4, 2 * RING, group, hl), BF),
            pltpu.VMEM((RING, RING, group // 2 // RING, hl), BF),
            pltpu.VMEM((4, 2, RING, group // RING, hl), BF),
            pltpu.VMEM((2, 2, group // RING, hl), F32),
            pltpu.VMEM((4, RING, sub, hid), BF),
            pltpu.VMEM((4, 2, sub // 2, hid), BF),
            pltpu.VMEM((4, 2, sub, hid), BF),
            pltpu.VMEM((4, sub, hid), F32),
            pltpu.VMEM((2, sub, hid), BF),
            pltpu.VMEM((2, sub, hid), BF),
            pltpu.VMEM((sub, hid), F32),
            pltpu.VMEM((2, hid, sub), F32),
            pltpu.VMEM((2, 8, 128), F32),
            pltpu.VMEM((8, 8, 128), F32),
            pltpu.VMEM((16, 8, 128), F32),
            pltpu.SemaphoreType.DMA((12,)),
            pltpu.SemaphoreType.DMA((111,)),
            pltpu.SemaphoreType.DMA((111,)),
        ],
        compiler_params=pltpu.CompilerParams(
            collective_id=0, has_side_effects=True, vmem_limit_bytes=67043328
        ),
    )(inputs, w_in[0], w_out[0], cotangent)
    steps = 4
    in_block = pl.BlockSpec((shard // steps, hid), lambda i: (i, 0))
    out_block = pl.BlockSpec((hid // steps, shard), lambda i: (i, 0))
    upd_in, upd_out = pl.pallas_call(
        clip,
        grid=(steps,),
        out_shape=(jax.ShapeDtypeStruct((shard, hid), F32), jax.ShapeDtypeStruct((hid, shard), F32)),
        in_specs=[pl.BlockSpec((1, 1), lambda i: (0, 0)), in_block, out_block],
        out_specs=(in_block, out_block),
    )(norm, tot_in, tot_out)
    return upd_in[None], upd_out[None], norm[0, 0]


def solution(mesh):
    split = Mesh(mesh.devices.reshape(mesh.shape["pipe"], 2, 2, RING, RING), AXES)
    placed = (
        P(None, DP, TENSOR),
        P("pipe", TENSOR_DP, None),
        P("pipe", None, TENSOR_DP),
        P(None, DP, TENSOR),
    )
    return jax.shard_map(
        on_device,
        mesh=split,
        in_specs=placed,
        out_specs=(P("pipe", TENSOR_DP, None), P("pipe", None, TENSOR_DP), P()),
        check_vma=False,
    )
```

```python
import jax
import jax.numpy as jnp
from jax import lax
from jax.experimental import pallas as pl
from jax.experimental.pallas import tpu as pltpu
from jax.sharding import Mesh
from jax.sharding import PartitionSpec as P

CLIP_NORM = 16384.0
AXES = ("pipe", "xhi", "core", "z", "y")
TENSOR = ("xhi", "core")
DP = ("z", "y")
PIPE_TENSOR_DP = ("pipe", "xhi", "core", "z", "y")
TENSOR_DP = ("xhi", "core", "z", "y")
MESH = pl.DeviceIdType.MESH
BF = jnp.bfloat16
F32 = jnp.float32

RING = 4
NT = (((1,), (1,)), ((), ()))
TN = (((0,), (0,)), ((), ()))


def kernel(
    x_hbm, win_hbm, wout_hbm, cot_hbm,
    tot_in, tot_out, norm_out,
    stage, x0, cot, x1, err1, raw, own, w, g, act, slope,
    part, r1, rx, r2, keep,
    rc, ra, rb,
    fin, pex, prx, late, turned, nsum, n1, n2,
    lsem, ssem, rsem,
):
    group, hid = part.shape[2], part.shape[3]
    rows = RING * group
    sub = w.shape[3]
    hl = hid // 2
    hs = sub // 2
    part_d = x0.shape[-1]
    tile = 256
    pipe = lax.axis_index("pipe")
    xhi = lax.axis_index("xhi")
    core = lax.axis_index("core")
    z = lax.axis_index("z")
    y = lax.axis_index("y")
    other = 1 - pipe
    core2 = 1 - core
    xi = xhi * 2 + pipe

    def turn(v, d):
        return lax.rem(v + d, RING)

    started = []
    count = [0]
    lcount = [0]

    class Outbox:

        def __init__(self, like):
            self.sem = ssem.at[len(started)]
            self.like = like
            started.append(self)

        def wait_send(self):
            sems, dev = self.last
            pltpu.make_async_remote_copy(
                src_ref=self.like, dst_ref=self.like, device_id=dev, device_id_type=MESH, **sems
            ).wait_send()

    class Group:
        def __init__(self, like, outbox=None):
            i = count[0]
            count[0] += 1
            if outbox is None:
                outbox = Outbox(like)
            self.sems = {"send_sem": outbox.sem, "recv_sem": rsem.at[i]}
            self.like, self.outbox = like, outbox

        def send(self, src, dst, dev):
            pltpu.make_async_remote_copy(
                src_ref=src, dst_ref=dst, device_id=dev, device_id_type=MESH, **self.sems
            ).start()
            self.whole = pltpu.make_async_remote_copy(
                src_ref=self.like, dst_ref=self.like, device_id=dev, device_id_type=MESH, **self.sems
            )
            self.outbox.last = self.sems, dev
            return self

        def wait_recv(self):
            self.whole.wait_recv()

    def remote(src, dst, dev):
        return Group(src).send(src, dst, dev)

    def same(ref, dev):
        return remote(ref, ref, dev)

    def group_of(like, items, outbox=None):
        made = Group(like, outbox)
        for src, dst, dev in items:
            made.send(src, dst, dev)
        return [made]

    class Local:
        def __init__(self, like):
            self.sem = lsem.at[lcount[0]]
            lcount[0] += 1
            self.whole = pltpu.make_async_copy(like, like, self.sem)

        def start(self, src, dst):
            pltpu.make_async_copy(src, dst, self.sem).start()
            return self

        def wait(self):
            self.whole.wait()

    def local(src, dst):
        return Local(dst).start(src, dst)

    def wait_all(copies):
        for copy in copies:
            copy.wait_recv()

    xpeers = []
    for code in (3, 2, 1):
        p_ = other if code % 2 else pipe
        h_ = 1 - xhi if code // 2 else xhi
        xpeers.append((code, {"pipe": p_, "xhi": h_}, h_ * 2 + p_))
    ypeers = [(d, {"y": turn(y, d)}, turn(y, d)) for d in (2, 1, 3)]
    zpeers = [(d, {"z": turn(z, d)}) for d in (1, 2, 3)]
    up, dn = {"z": turn(z, 1)}, {"z": turn(z, 3)}
    zu, zd, z2 = turn(z, 1), turn(z, 3), turn(z, 2)
    twin = {"core": core2}
    pair = {"pipe": other}
    ycore = [(d * 2, {**dev}, yy, core) for d, dev, yy in ypeers]
    ycore += [(d * 2 + 1, {**dev, "core": core2}, yy, core2) for d, dev, yy in ypeers]
    ycore += [(1, twin, y, core2)]
    xz = [(code, dev) for code, dev, _ in xpeers]
    xz += [(d * 4, dev) for d, dev in zpeers]
    xz += [(d * 4 + code, {**dx, **dz}) for d, dz in zpeers for code, dx, _ in xpeers]

    keep_rows = pl.ds(pl.multiple_of(pipe * sub, sub), sub)
    give_rows = pl.ds(pl.multiple_of(other * sub, sub), sub)
    out_load = [
        local(wout_hbm.at[:, give_rows], raw.at[0]),
        local(wout_hbm.at[:, keep_rows], raw.at[1]),
    ]
    own_load = [
        local(win_hbm.at[give_rows, :], own.at[0]),
        local(win_hbm.at[keep_rows, :], w.at[2 * pipe, core, z]),
    ]

    def fetch(src, n):
        copies = Local(stage.at[n])
        for yy in range(RING):
            for zz in range(RING):
                off = pl.multiple_of((zz * RING + yy) * 2 * sub + pipe * sub, sub)
                copies.start(src.at[:, :, pl.ds(off, sub)], stage.at[n, yy, :, :, pl.ds(zz * sub, sub)])
        return copies

    x_load = fetch(x_hbm, 0)
    cot_load = fetch(cot_hbm, 1)

    barrier = pltpu.get_barrier_semaphore()
    peers = [dev for _, dev, _, _ in ycore] + [dev for _, dev in xz]
    for dev in peers:
        pl.semaphore_signal(barrier, inc=1, device_id=dev, device_id_type=MESH)
    for copy in out_load:
        copy.wait()
    own[1] = raw[0].T
    w[2 * pipe + 1, core, z] = raw[1].T
    pl.semaphore_wait(barrier, len(peers))

    half_tok = x0.shape[2]
    my_cols = pl.ds(pl.multiple_of(core * (part_d // 2), part_d // 2), part_d // 2)

    def swap_tokens(n, dst):
        def piece(yy, cc):
            toks = pl.ds(pl.multiple_of(cc * half_tok, half_tok), half_tok)
            return stage.at[n, yy, :, toks, :]

        landing = dst.at[y, :, :, my_cols]
        return local(piece(y, core), landing), group_of(
            r1.at[n, pl.ds(1, 7)], [(piece(yy, cc), landing, dev) for _, dev, yy, cc in ycore]
        )

    lo, hi = pl.ds(0, hs), pl.ds(hs, hs)

    def g1(k, rows_of=slice(None)):
        ref = w.at[k, core, z, rows_of, :]
        return group_of(w.at[k, core, pl.ds(0, 2), rows_of, :], [(ref, ref, up), (ref, ref, dn)])

    def g2(k):
        a, b = w.at[k, core, zd, lo, :], w.at[k, core, zu, hi, :]
        return group_of(w.at[k, core, z], [(a, a, up), (b, b, dn)])

    def g2c(k):
        refs = [w.at[k, core, at] for at in (z, zu, zd)]
        return group_of(w.at[k, core, pl.ds(0, 3)], [(ref, ref, twin) for ref in refs])

    def g3(k):
        return [same(w.at[k, core, z2], twin)]

    halves = (pl.ds(0, hl), pl.ds(hl, hl))

    mrows = group // 2
    streams = (pl.ds(0, mrows), pl.ds(mrows, mrows))
    srows = RING * mrows

    def project(src, k, ph, half, m):
        cols = halves[half]
        left = src[:, m].reshape(srows, part_d)
        right = w[k, :, :, :, cols].reshape(part_d, hl)
        got = jnp.dot(left, right, preferred_element_type=F32)
        part[ph, :, streams[m], cols] = got.astype(BF).reshape(RING, mrows, hl)

    def widen(base, units_ref, k, out, m):
        for cc in range(2):
            cols = pl.ds(cc * RING * sub, RING * sub)
            left = units_ref[:, streams[m], :].reshape(srows, hid)
            right = w[k, cc].reshape(RING * sub, hid)
            add = lax.dot_general(left, right, NT, preferred_element_type=F32)
            old = base[:, m, :, cols].reshape(srows, RING * sub).astype(F32)
            out[:, m, :, cols] = (old + add).astype(BF).reshape(RING, mrows, RING * sub)

    def weight_grad(left_ref, right, k):
        def side(cc):
            cols = pl.ds(pl.multiple_of(cc * RING * sub, tile), RING * sub)
            left = left_ref[:, :, :, cols].reshape(rows, RING * sub)
            got = lax.dot_general(left, right[...].reshape(rows, hid), TN, preferred_element_type=F32)
            g[k, cc] = got.astype(BF).reshape(RING, sub, hid)

        def across(p):
            zz = pl.ds(pl.multiple_of(p * 2, 2), 2)
            return remote(g.at[k, core2, zz], rc.at[k, zz], twin)

        p_far = z2 // 2
        p_near = 1 - p_far
        side(core2)
        far = across(p_far)
        near = across(p_near)
        side(core)
        return q1(k, [far]), near

    def plus(x, *more):
        total = x.astype(F32)
        for m in more:
            total = total + m.astype(F32)
        return total

    first = (xpeers, ypeers)
    second = (ypeers, xpeers)
    block = (xi, y)
    inner = (y, xi)

    crows = mrows // RING

    def inner_rows(at, m):
        return pl.ds(pl.multiple_of(m * mrows + at * crows, crows), crows)

    def slots(m):
        return pl.ds(m * crows, crows)

    big = r1.at[:, pl.ds(0, 6)]
    small = r2.at[:, :, pl.ds(0, 3)]
    r1_out, r2_out, s1_out, s2_out = Outbox(big), Outbox(small), Outbox(small), Outbox(big)

    def r1_at(half, slot):
        return half * RING + slot

    def rs1(ph, half, m):
        lanes, r = halves[half], streams[m]
        return group_of(
            r1.at[ph, pl.ds(r1_at(half, 1), 3), r],
            [
                (part.at[ph, at, r, lanes], r1.at[ph, r1_at(half, slot), r], dev)
                for slot, dev, at in first[half]
            ],
            r1_out,
        )

    def rs2(ph, half, m, copies):
        wait_all(copies)
        lanes, r = halves[half], streams[m]
        b = block[half]
        part[ph, b, r, lanes] = plus(
            part[ph, b, r, lanes], *[r1[ph, r1_at(half, slot), r] for slot in (1, 2, 3)]
        ).astype(BF)
        return group_of(
            r2.at[ph, half, pl.ds(1, 3), slots(m)],
            [
                (part.at[ph, b, inner_rows(at, m), lanes], r2.at[ph, half, slot, slots(m)], dev)
                for slot, dev, at in second[half]
            ],
            r2_out,
        )

    def rs1_turned(ph, m):
        return group_of(
            rx.at[pl.ds(1, 3)],
            [(part.at[ph, :, inner_rows(at, m), halves[1]], rx.at[slot], dev) for slot, dev, at in xpeers],
            r1_out,
        )

    def rs2_turned(ph, m, copies):
        wait_all(copies)
        mid = inner_rows(xi, m)
        part[ph, :, mid, halves[1]] = plus(part[ph, :, mid, halves[1]], rx[1], rx[2], rx[3]).astype(BF)
        return group_of(
            r2.at[ph, 1, pl.ds(1, 3), slots(m)],
            [(part.at[ph, at, mid, halves[1]], r2.at[ph, 1, slot, slots(m)], dev) for slot, dev, at in ypeers],
            r2_out,
        )

    def units(ph, half, m, copies):
        wait_all(copies)
        c = slots(m)
        return plus(
            part[ph, block[half], inner_rows(inner[half], m), halves[half]],
            r2[ph, half, 1, c], r2[ph, half, 2, c], r2[ph, half, 3, c],
        )

    def put(ref, half, m, value):
        ref[block[half], inner_rows(inner[half], m), halves[half]] = value

    def sp1(ref, half, m):
        piece = ref.at[block[half], inner_rows(inner[half], m), halves[half]]
        like = ref.at[block[half], pl.ds(m * mrows, 3 * crows), halves[half]]
        return group_of(like, [(piece, piece, dev) for _, dev, _ in second[half]], s1_out)

    def sp2(ref, half, m, copies):
        wait_all(copies)
        piece = ref.at[block[half], streams[m], halves[half]]
        like = ref.at[pl.ds(0, 3), streams[m], halves[half]]
        return group_of(like, [(piece, piece, dev) for _, dev, _ in first[half]], s2_out)

    def slope_of(upward, pre):
        sig = jax.nn.sigmoid(pre)
        return (upward * sig * (1.0 + pre * (1.0 - sig))).astype(BF)

    q1_out, q2_out = Outbox(ra), Outbox(rb)

    def q1(k, copies):
        wait_all(copies)
        g[k, core, z2] = plus(g[k, core, z2], rc[k, z2]).astype(BF)
        return group_of(
            ra.at[k],
            [
                (g.at[k, core, z2, lo, :], ra.at[k, 0], up),
                (g.at[k, core, z2, hi, :], ra.at[k, 1], dn),
            ],
            q1_out,
        )

    def q2(k, copies, near):
        near.wait_recv()
        g[k, core, zu, hi, :] = plus(g[k, core, zu, hi, :], rc[k, zu, hi, :]).astype(BF)
        g[k, core, zd, lo, :] = plus(g[k, core, zd, lo, :], rc[k, zd, lo, :]).astype(BF)
        wait_all(copies)
        g[k, core, zu, lo, :] = plus(g[k, core, zu, lo, :], rc[k, zu, lo, :], ra[k, 0]).astype(BF)
        g[k, core, zd, hi, :] = plus(g[k, core, zd, hi, :], rc[k, zd, hi, :], ra[k, 1]).astype(BF)
        return group_of(
            rb.at[k],
            [(g.at[k, core, zu], rb.at[k, 0], up), (g.at[k, core, zd], rb.at[k, 1], dn)],
            q2_out,
        )

    def fold(value):
        lanes = value.shape[-1]
        value = value.reshape(sub // 8, 8, lanes).sum(0)
        total = value[:, 0:128]
        for i in range(1, lanes // 128):
            total = total + value[:, i * 128 : (i + 1) * 128]
        return total

    def finish(k, copies):
        wait_all(copies)
        value = plus(g[k, core, z], rc[k, z], rb[k, 0], rb[k, 1])
        fin[k] = value
        return fold(value * value)

    def hand_over(kind):
        pex[kind] = fin[2 * other + kind].astype(BF)
        return remote(pex.at[kind], prx.at[kind], pair)

    HALVES = (0, 1)

    def both(f):
        return [f(half) for half in HALVES]

    def project_send(src, k, ph, m):
        sent = []
        for half in HALVES:
            project(src, k, ph, half, m)
            sent.append(rs1(ph, half, m))
        return sent

    def all_rs2(ph, m, sent):
        return both(lambda half: rs2(ph, half, m, sent[half]))

    def all_sp2(ref, m, sent):
        return both(lambda half: sp2(ref, half, m, sent[half]))

    def settle(sent):
        for copies in sent:
            wait_all(copies)

    quarter = sub // 4
    cuts = [pl.ds(i * quarter, quarter) for i in range(4)]
    order = (0, 2, 1, 3)
    def open_act(m, sent):
        done = []
        for half in HALVES:
            pre = units(0, half, m, sent[half])
            keep[0, half, slots(m), :] = pre
            put(act.at[0], half, m, jax.nn.silu(pre).astype(BF))
            done.append(sp1(act.at[0], half, m))
        return done

    own1, got1 = 1 + pipe, 1 + other
    for copy in own_load:
        copy.wait()
    e0 = {i: remote(own.at[pipe, cuts[i], :], w.at[3 * pipe, core, z, cuts[i], :], pair) for i in order}
    e1 = remote(own.at[other], w.at[own1, core, z], pair)
    x_load.wait()
    x_here, x_swap = swap_tokens(0, x0)
    ca_own1 = g1(own1, lo)
    cot_load.wait()
    cot_here, cot_swap = swap_tokens(1, cot)
    ca0 = {}
    for i in order:
        e0[i].wait_recv()
        ca0[i] = g1(0, cuts[i])
    cb0 = Group(w.at[0, core, z])
    for i in order:
        wait_all(ca0[i])
        ahead, to = (zd, up) if i < 2 else (zu, dn)
        ref = w.at[0, core, ahead, cuts[i], :]
        cb0.send(ref, ref, to)
    cc0 = g2c(0)
    ca3 = g1(3)
    ca_own1 += g1(own1, hi)
    e1.wait_recv()
    ca_got1 = g1(got1)
    cb0.wait_recv()
    cd0 = g3(0)
    x_here.wait()
    wait_all(x_swap)
    wait_all(cc0)
    wait_all(cd0)

    project(x0, 0, 0, 0, 0)
    p00a = rs1(0, 0, 0)
    project(x0, 0, 0, 1, 0)
    p00b = rs1_turned(0, 0)
    p01 = project_send(x0, 0, 0, 1)
    wait_all(ca3)
    cb3 = g2(3)
    cc3 = g2c(3)
    wait_all(ca_own1)
    cb_own1 = g2(own1)
    cc_own1 = g2c(own1)
    p00 = [rs2(0, 0, 0, p00a), rs2_turned(0, 0, p00b)]
    p01 = all_rs2(0, 1, p01)
    a00 = open_act(0, p00)
    wait_all(ca_got1)
    cb_got1 = g2(got1)
    cc_got1 = g2c(got1)
    a01 = open_act(1, p01)
    a00 = all_sp2(act.at[0], 0, a00)
    wait_all(cb3)
    cd3 = g3(3)
    a01 = all_sp2(act.at[0], 1, a01)
    cot_here.wait()
    wait_all(cot_swap)
    wait_all(cc3)
    wait_all(cd3)
    p20 = project_send(cot, 3, 2, 0)
    p21 = project_send(cot, 3, 2, 1)
    wait_all(cb_own1)
    cd_own1 = g3(own1)
    wait_all(cb_got1)
    cd_got1 = g3(got1)
    settle(a00)
    wait_all(cc_own1 + cc_got1)
    wait_all(cd_own1 + cd_got1)
    widen(x0, act.at[0], 1, x1, 0)
    p10 = project_send(x1, 2, 1, 0)
    settle(a01)
    widen(x0, act.at[0], 1, x1, 1)
    p11 = project_send(x1, 2, 1, 1)
    p20 = all_rs2(2, 0, p20)
    p21 = all_rs2(2, 1, p21)
    p10 = all_rs2(1, 0, p10)
    def open_slope(m, sent_up, sent_pre):
        done = []
        for half in HALVES:
            upward = units(2, half, m, sent_up[half])
            pre = units(1, half, m, sent_pre[half])
            put(slope.at[1], half, m, slope_of(upward, pre))
            done.append(sp1(slope.at[1], half, m))
            put(act.at[1], half, m, jax.nn.silu(pre).astype(BF))
        return done

    p11 = all_rs2(1, 1, p11)
    s10 = open_slope(0, p20, p10)
    s11 = open_slope(1, p21, p11)
    s10 = all_sp2(slope.at[1], 0, s10)
    s11 = all_sp2(slope.at[1], 1, s11)
    a10 = both(lambda half: sp1(act.at[1], half, 0))
    a11 = both(lambda half: sp1(act.at[1], half, 1))
    settle(s10)
    widen(cot, slope.at[1], 2, err1, 0)
    p30 = project_send(err1, 1, 3, 0)
    settle(s11)
    widen(cot, slope.at[1], 2, err1, 1)
    p31 = project_send(err1, 1, 3, 1)
    a10 = all_sp2(act.at[1], 0, a10)
    d2, near2 = weight_grad(x1, slope.at[1], 2)
    p30 = all_rs2(3, 0, p30)
    p31 = all_rs2(3, 1, p31)
    a11 = all_sp2(act.at[1], 1, a11)
    d1, near1 = weight_grad(err1, act.at[0], 1)
    d2 = q2(2, d2, near2)
    def close_slope(m, sent):
        done = []
        for half in HALVES:
            upward = units(3, half, m, sent[half])
            put(slope.at[0], half, m, slope_of(upward, keep[0, half, slots(m), :]))
            done.append(sp1(slope.at[0], half, m))
        return done

    s00 = close_slope(0, p30)
    s01 = close_slope(1, p31)
    settle(a10)
    settle(a11)
    d3, near3 = weight_grad(cot, act.at[1], 3)
    s00 = all_sp2(slope.at[0], 0, s00)
    s01 = all_sp2(slope.at[0], 1, s01)
    d1 = q2(1, d1, near1)
    squares = finish(2, d2)
    settle(s00)
    settle(s01)
    d0, near0 = weight_grad(x0, slope.at[0], 0)
    d3 = q2(3, d3, near3)
    squares = squares + finish(1, d1)
    d0 = q2(0, d0, near0)
    squares = squares + finish(3, d3)
    h1 = hand_over(1)
    turned[0] = fin[2 * pipe + 1].T
    writes = [local(turned.at[0], tot_out.at[:, keep_rows])]
    squares = squares + finish(0, d0)
    nsum[0] = squares
    c1 = group_of(n2.at[pl.ds(1, 15)], [(nsum.at[0], n2.at[code], dev) for code, dev in xz])
    h0 = hand_over(0)
    writes.append(local(fin.at[2 * pipe], tot_in.at[keep_rows, :]))
    wait_all(c1)
    total = nsum[0]
    for code in range(1, 16):
        total = total + n2[code]
    nsum[1] = total
    c2 = group_of(n1.at[pl.ds(1, 7)], [(nsum.at[1], n1.at[code], dev) for code, dev, _, _ in ycore])
    h1.wait_recv()
    turned[1] = prx[1].astype(F32).T
    writes.append(local(turned.at[1], tot_out.at[:, give_rows]))
    wait_all(c2)
    total = nsum[1]
    for code in range(1, 8):
        total = total + n1[code]
    norm = jnp.sqrt(jnp.sum(total, keepdims=True))
    norm_out[...] = norm
    h0.wait_recv()
    late[...] = prx[0].astype(F32)
    writes.append(local(late, tot_in.at[give_rows, :]))
    for copy in started:
        copy.wait_send()
    for copy in writes:
        copy.wait()


def clip(norm_ref, tot_in, tot_out, upd_in, upd_out):
    factor = jnp.minimum(1.0, CLIP_NORM / norm_ref[...])
    upd_in[...] = tot_in[...] * factor
    upd_out[...] = tot_out[...] * factor


def on_device(inputs, w_in, w_out, cotangent):
    micro, tok, cols = inputs.shape
    shard, hid = w_in.shape[1], w_in.shape[2]
    sub = shard // 2
    part_d = cols // 4
    group = micro * tok // 2
    hl = hid // 2
    any_spec = pl.BlockSpec(memory_space=pl.ANY)
    vmem = pl.BlockSpec(memory_space=pltpu.VMEM)
    tokens = pltpu.VMEM((RING, micro, tok // 2, part_d), BF)
    weights = pltpu.VMEM((4, 2, RING, sub, hid), BF)
    layers = pltpu.VMEM((2, RING, group, hid), BF)
    tot_in, tot_out, norm = pl.pallas_call(
        kernel,
        out_shape=(
            jax.ShapeDtypeStruct((shard, hid), F32),
            jax.ShapeDtypeStruct((hid, shard), F32),
            jax.ShapeDtypeStruct((1, 1), F32),
        ),
        in_specs=[any_spec] * 4,
        out_specs=(any_spec, any_spec, vmem),
        scratch_shapes=[
            pltpu.VMEM((2, RING, micro, tok, RING * sub), BF),
            tokens, tokens, tokens, tokens,
            pltpu.VMEM((2, hid, sub), BF),
            pltpu.VMEM((2, sub, hid), BF),
            weights, weights, layers, layers,
            pltpu.VMEM((4, RING, group, hid), BF),
            pltpu.VMEM((4, 2 * RING, group, hl), BF),
            pltpu.VMEM((RING, RING, group // 2 // RING, hl), BF),
            pltpu.VMEM((4, 2, RING, group // RING, hl), BF),
            pltpu.VMEM((2, 2, group // RING, hl), F32),
            pltpu.VMEM((4, RING, sub, hid), BF),
            pltpu.VMEM((4, 2, sub // 2, hid), BF),
            pltpu.VMEM((4, 2, sub, hid), BF),
            pltpu.VMEM((4, sub, hid), F32),
            pltpu.VMEM((2, sub, hid), BF),
            pltpu.VMEM((2, sub, hid), BF),
            pltpu.VMEM((sub, hid), F32),
            pltpu.VMEM((2, hid, sub), F32),
            pltpu.VMEM((2, 8, 128), F32),
            pltpu.VMEM((8, 8, 128), F32),
            pltpu.VMEM((16, 8, 128), F32),
            pltpu.SemaphoreType.DMA((12,)),
            pltpu.SemaphoreType.DMA((45,)),
            pltpu.SemaphoreType.DMA((111,)),
        ],
        compiler_params=pltpu.CompilerParams(
            collective_id=0, has_side_effects=True, vmem_limit_bytes=67043328
        ),
    )(inputs, w_in[0], w_out[0], cotangent)
    steps = 2
    in_block = pl.BlockSpec((shard // steps, hid), lambda i: (i, 0))
    out_block = pl.BlockSpec((hid // steps, shard), lambda i: (i, 0))
    upd_in, upd_out = pl.pallas_call(
        clip,
        grid=(steps,),
        out_shape=(jax.ShapeDtypeStruct((shard, hid), F32), jax.ShapeDtypeStruct((hid, shard), F32)),
        in_specs=[pl.BlockSpec((1, 1), lambda i: (0, 0)), in_block, out_block],
        out_specs=(in_block, out_block),
    )(norm, tot_in, tot_out)
    return upd_in[None], upd_out[None], norm[0, 0]


def solution(mesh):
    split = Mesh(mesh.devices.reshape(mesh.shape["pipe"], 2, 2, RING, RING), AXES)
    placed = (
        P(None, DP, TENSOR),
        P("pipe", TENSOR_DP, None),
        P("pipe", None, TENSOR_DP),
        P(None, DP, TENSOR),
    )
    return jax.shard_map(
        on_device,
        mesh=split,
        in_specs=placed,
        out_specs=(P("pipe", TENSOR_DP, None), P("pipe", None, TENSOR_DP), P()),
        check_vma=False,
    )
```

```python
import jax
import jax.numpy as jnp
from jax import lax
from jax.experimental import pallas as pl
from jax.experimental.pallas import tpu as pltpu
from jax.sharding import Mesh
from jax.sharding import PartitionSpec as P

CLIP_NORM = 16384.0
AXES = ("pipe", "xhi", "core", "z", "y")
TENSOR = ("xhi", "core")
DP = ("z", "y")
PIPE_TENSOR_DP = ("pipe", "xhi", "core", "z", "y")
TENSOR_DP = ("xhi", "core", "z", "y")
MESH = pl.DeviceIdType.MESH
BF = jnp.bfloat16
F32 = jnp.float32

RING = 4
NT = (((1,), (1,)), ((), ()))
TN = (((0,), (0,)), ((), ()))


def kernel(
    x_hbm, win_hbm, wout_hbm, cot_hbm,
    tot_in, tot_out, norm_out,
    stage, x0, cot, x1, err1, raw, own, w, g, act, slope,
    part, r1, rx, r2, keep,
    rc, ra, rb,
    fin, pex, prx, late, turned, nsum, n1, n2,
    lsem, ssem, rsem,
):
    group, hid = part.shape[2], part.shape[3]
    rows = RING * group
    sub = w.shape[3]
    hl = hid // 2
    hs = sub // 2
    part_d = x0.shape[-1]
    tile = 256
    pipe = lax.axis_index("pipe")
    xhi = lax.axis_index("xhi")
    core = lax.axis_index("core")
    z = lax.axis_index("z")
    y = lax.axis_index("y")
    other = 1 - pipe
    core2 = 1 - core
    xi = xhi * 2 + pipe

    def turn(v, d):
        return lax.rem(v + d, RING)

    started = []
    count = [0]
    lcount = [0]

    class Outbox:

        def __init__(self, like):
            self.sem = ssem.at[len(started)]
            self.like = like
            started.append(self)

        def wait_send(self):
            sems, dev = self.last
            pltpu.make_async_remote_copy(
                src_ref=self.like, dst_ref=self.like, device_id=dev, device_id_type=MESH, **sems
            ).wait_send()

    class Group:
        def __init__(self, like, outbox=None):
            i = count[0]
            count[0] += 1
            if outbox is None:
                outbox = Outbox(like)
            self.sems = {"send_sem": outbox.sem, "recv_sem": rsem.at[i]}
            self.like, self.outbox = like, outbox

        def send(self, src, dst, dev):
            pltpu.make_async_remote_copy(
                src_ref=src, dst_ref=dst, device_id=dev, device_id_type=MESH, **self.sems
            ).start()
            self.whole = pltpu.make_async_remote_copy(
                src_ref=self.like, dst_ref=self.like, device_id=dev, device_id_type=MESH, **self.sems
            )
            self.outbox.last = self.sems, dev
            return self

        def wait_recv(self):
            self.whole.wait_recv()

    def remote(src, dst, dev):
        return Group(src).send(src, dst, dev)

    def same(ref, dev):
        return remote(ref, ref, dev)

    def group_of(like, items, outbox=None):
        made = Group(like, outbox)
        for src, dst, dev in items:
            made.send(src, dst, dev)
        return [made]

    class Local:
        def __init__(self, like):
            self.sem = lsem.at[lcount[0]]
            lcount[0] += 1
            self.whole = pltpu.make_async_copy(like, like, self.sem)

        def start(self, src, dst):
            pltpu.make_async_copy(src, dst, self.sem).start()
            return self

        def wait(self):
            self.whole.wait()

    def local(src, dst):
        return Local(dst).start(src, dst)

    def wait_all(copies):
        for copy in copies:
            copy.wait_recv()

    xpeers = []
    for code in (3, 2, 1):
        p_ = other if code % 2 else pipe
        h_ = 1 - xhi if code // 2 else xhi
        xpeers.append((code, {"pipe": p_, "xhi": h_}, h_ * 2 + p_))
    ypeers = [(d, {"y": turn(y, d)}, turn(y, d)) for d in (2, 1, 3)]
    zpeers = [(d, {"z": turn(z, d)}) for d in (1, 2, 3)]
    up, dn = {"z": turn(z, 1)}, {"z": turn(z, 3)}
    zu, zd, z2 = turn(z, 1), turn(z, 3), turn(z, 2)
    twin = {"core": core2}
    pair = {"pipe": other}
    ycore = [(d * 2, {**dev}, yy, core) for d, dev, yy in ypeers]
    ycore += [(d * 2 + 1, {**dev, "core": core2}, yy, core2) for d, dev, yy in ypeers]
    ycore += [(1, twin, y, core2)]
    xz = [(code, dev) for code, dev, _ in xpeers]
    xz += [(d * 4, dev) for d, dev in zpeers]
    xz += [(d * 4 + code, {**dx, **dz}) for d, dz in zpeers for code, dx, _ in xpeers]

    keep_rows = pl.ds(pl.multiple_of(pipe * sub, sub), sub)
    give_rows = pl.ds(pl.multiple_of(other * sub, sub), sub)
    out_load = [
        local(wout_hbm.at[:, give_rows], raw.at[0]),
        local(wout_hbm.at[:, keep_rows], raw.at[1]),
    ]
    own_load = [
        local(win_hbm.at[give_rows, :], own.at[0]),
        local(win_hbm.at[keep_rows, :], w.at[2 * pipe, core, z]),
    ]

    def fetch(src, n):
        copies = Local(stage.at[n])
        for yy in range(RING):
            for zz in range(RING):
                off = pl.multiple_of((zz * RING + yy) * 2 * sub + pipe * sub, sub)
                copies.start(src.at[:, :, pl.ds(off, sub)], stage.at[n, yy, :, :, pl.ds(zz * sub, sub)])
        return copies

    x_load = fetch(x_hbm, 0)
    cot_load = fetch(cot_hbm, 1)

    barrier = pltpu.get_barrier_semaphore()
    peers = [dev for _, dev, _, _ in ycore] + [dev for _, dev in xz]
    for dev in peers:
        pl.semaphore_signal(barrier, inc=1, device_id=dev, device_id_type=MESH)
    for copy in out_load:
        copy.wait()
    own[1] = raw[0].T
    w[2 * pipe + 1, core, z] = raw[1].T
    pl.semaphore_wait(barrier, len(peers))

    half_tok = x0.shape[2]
    my_cols = pl.ds(pl.multiple_of(core * (part_d // 2), part_d // 2), part_d // 2)

    def swap_tokens(n, dst):
        def piece(yy, cc):
            toks = pl.ds(pl.multiple_of(cc * half_tok, half_tok), half_tok)
            return stage.at[n, yy, :, toks, :]

        landing = dst.at[y, :, :, my_cols]
        return local(piece(y, core), landing), group_of(
            r1.at[n, pl.ds(1, 7)], [(piece(yy, cc), landing, dev) for _, dev, yy, cc in ycore]
        )

    lo, hi = pl.ds(0, hs), pl.ds(hs, hs)

    def g1(k, rows_of=slice(None)):
        ref = w.at[k, core, z, rows_of, :]
        return group_of(w.at[k, core, pl.ds(0, 2), rows_of, :], [(ref, ref, up), (ref, ref, dn)])

    def g2(k):
        a, b = w.at[k, core, zd, lo, :], w.at[k, core, zu, hi, :]
        return group_of(w.at[k, core, z], [(a, a, up), (b, b, dn)])

    def g2c(k):
        refs = [w.at[k, core, at] for at in (z, zu, zd)]
        return group_of(w.at[k, core, pl.ds(0, 3)], [(ref, ref, twin) for ref in refs])

    def g3(k):
        return [same(w.at[k, core, z2], twin)]

    halves = (pl.ds(0, hl), pl.ds(hl, hl))

    mrows = group // 2
    streams = (pl.ds(0, mrows), pl.ds(mrows, mrows))
    srows = RING * mrows

    def project(src, k, ph, half, m):
        cols = halves[half]
        left = src[:, m].reshape(srows, part_d)
        right = w[k, :, :, :, cols].reshape(part_d, hl)
        got = jnp.dot(left, right, preferred_element_type=F32)
        part[ph, :, streams[m], cols] = got.astype(BF).reshape(RING, mrows, hl)

    def widen(base, units_ref, k, out, m):
        for cc in range(2):
            cols = pl.ds(cc * RING * sub, RING * sub)
            left = units_ref[:, streams[m], :].reshape(srows, hid)
            right = w[k, cc].reshape(RING * sub, hid)
            add = lax.dot_general(left, right, NT, preferred_element_type=F32)
            old = base[:, m, :, cols].reshape(srows, RING * sub).astype(F32)
            out[:, m, :, cols] = (old + add).astype(BF).reshape(RING, mrows, RING * sub)

    def weight_grad(left_ref, right, k):
        def side(cc):
            cols = pl.ds(pl.multiple_of(cc * RING * sub, tile), RING * sub)
            left = left_ref[:, :, :, cols].reshape(rows, RING * sub)
            got = lax.dot_general(left, right[...].reshape(rows, hid), TN, preferred_element_type=F32)
            g[k, cc] = got.astype(BF).reshape(RING, sub, hid)

        def across(p):
            zz = pl.ds(pl.multiple_of(p * 2, 2), 2)
            return remote(g.at[k, core2, zz], rc.at[k, zz], twin)

        p_far = z2 // 2
        p_near = 1 - p_far
        side(core2)
        far = across(p_far)
        near = across(p_near)
        side(core)
        return [far], near

    def plus(x, *more):
        total = x.astype(F32)
        for m in more:
            total = total + m.astype(F32)
        return total

    first = (xpeers, ypeers)
    second = (ypeers, xpeers)
    block = (xi, y)
    inner = (y, xi)

    crows = mrows // RING

    def inner_rows(at, m):
        return pl.ds(pl.multiple_of(m * mrows + at * crows, crows), crows)

    def slots(m):
        return pl.ds(m * crows, crows)

    big = r1.at[:, pl.ds(0, 6)]
    small = r2.at[:, :, pl.ds(0, 3)]
    r1_out, r2_out, s1_out, s2_out = Outbox(big), Outbox(small), Outbox(small), Outbox(big)

    def r1_at(half, slot):
        return half * RING + slot

    def rs1(ph, half, m):
        lanes, r = halves[half], streams[m]
        return group_of(
            r1.at[ph, pl.ds(r1_at(half, 1), 3), r],
            [
                (part.at[ph, at, r, lanes], r1.at[ph, r1_at(half, slot), r], dev)
                for slot, dev, at in first[half]
            ],
            r1_out,
        )

    def rs2(ph, half, m, copies):
        wait_all(copies)
        lanes, r = halves[half], streams[m]
        b = block[half]
        part[ph, b, r, lanes] = plus(
            part[ph, b, r, lanes], *[r1[ph, r1_at(half, slot), r] for slot in (1, 2, 3)]
        ).astype(BF)
        return group_of(
            r2.at[ph, half, pl.ds(1, 3), slots(m)],
            [
                (part.at[ph, b, inner_rows(at, m), lanes], r2.at[ph, half, slot, slots(m)], dev)
                for slot, dev, at in second[half]
            ],
            r2_out,
        )

    def rs1_turned(ph, m):
        return group_of(
            rx.at[pl.ds(1, 3)],
            [(part.at[ph, :, inner_rows(at, m), halves[1]], rx.at[slot], dev) for slot, dev, at in xpeers],
            r1_out,
        )

    def rs2_turned(ph, m, copies):
        wait_all(copies)
        mid = inner_rows(xi, m)
        part[ph, :, mid, halves[1]] = plus(part[ph, :, mid, halves[1]], rx[1], rx[2], rx[3]).astype(BF)
        return group_of(
            r2.at[ph, 1, pl.ds(1, 3), slots(m)],
            [(part.at[ph, at, mid, halves[1]], r2.at[ph, 1, slot, slots(m)], dev) for slot, dev, at in ypeers],
            r2_out,
        )

    def units(ph, half, m, copies):
        wait_all(copies)
        c = slots(m)
        return plus(
            part[ph, block[half], inner_rows(inner[half], m), halves[half]],
            r2[ph, half, 1, c], r2[ph, half, 2, c], r2[ph, half, 3, c],
        )

    def put(ref, half, m, value):
        ref[block[half], inner_rows(inner[half], m), halves[half]] = value

    def sp1(ref, half, m):
        piece = ref.at[block[half], inner_rows(inner[half], m), halves[half]]
        like = ref.at[block[half], pl.ds(m * mrows, 3 * crows), halves[half]]
        return group_of(like, [(piece, piece, dev) for _, dev, _ in second[half]], s1_out)

    def sp2(ref, half, m, copies):
        wait_all(copies)
        piece = ref.at[block[half], streams[m], halves[half]]
        like = ref.at[pl.ds(0, 3), streams[m], halves[half]]
        return group_of(like, [(piece, piece, dev) for _, dev, _ in first[half]], s2_out)

    def slope_of(upward, pre):
        sig = jax.nn.sigmoid(pre)
        return (upward * sig * (1.0 + pre * (1.0 - sig))).astype(BF)

    q1_out, q2_out = Outbox(ra), Outbox(rb)

    def q1(k, copies):
        wait_all(copies)
        g[k, core, z2] = plus(g[k, core, z2], rc[k, z2]).astype(BF)
        return group_of(
            ra.at[k],
            [
                (g.at[k, core, z2, lo, :], ra.at[k, 0], up),
                (g.at[k, core, z2, hi, :], ra.at[k, 1], dn),
            ],
            q1_out,
        )

    def q2(k, copies, near):
        near.wait_recv()
        g[k, core, zu, hi, :] = plus(g[k, core, zu, hi, :], rc[k, zu, hi, :]).astype(BF)
        g[k, core, zd, lo, :] = plus(g[k, core, zd, lo, :], rc[k, zd, lo, :]).astype(BF)
        wait_all(copies)
        g[k, core, zu, lo, :] = plus(g[k, core, zu, lo, :], rc[k, zu, lo, :], ra[k, 0]).astype(BF)
        g[k, core, zd, hi, :] = plus(g[k, core, zd, hi, :], rc[k, zd, hi, :], ra[k, 1]).astype(BF)
        return group_of(
            rb.at[k],
            [(g.at[k, core, zu], rb.at[k, 0], up), (g.at[k, core, zd], rb.at[k, 1], dn)],
            q2_out,
        )

    def fold(value):
        lanes = value.shape[-1]
        value = value.reshape(sub // 8, 8, lanes).sum(0)
        total = value[:, 0:128]
        for i in range(1, lanes // 128):
            total = total + value[:, i * 128 : (i + 1) * 128]
        return total

    def finish(k, copies):
        wait_all(copies)
        value = plus(g[k, core, z], rc[k, z], rb[k, 0], rb[k, 1])
        fin[k] = value
        return fold(value * value)

    def hand_over(kind):
        pex[kind] = fin[2 * other + kind].astype(BF)
        return remote(pex.at[kind], prx.at[kind], pair)

    HALVES = (0, 1)

    def both(f):
        return [f(half) for half in HALVES]

    def project_send(src, k, ph, m):
        sent = []
        for half in HALVES:
            project(src, k, ph, half, m)
            sent.append(rs1(ph, half, m))
        return sent

    def all_rs2(ph, m, sent):
        return both(lambda half: rs2(ph, half, m, sent[half]))

    def all_sp2(ref, m, sent):
        return both(lambda half: sp2(ref, half, m, sent[half]))

    def settle(sent):
        for copies in sent:
            wait_all(copies)

    quarter = sub // 4
    cuts = [pl.ds(i * quarter, quarter) for i in range(4)]
    order = (0, 2, 1, 3)
    def open_act(m, sent):
        done = []
        for half in HALVES:
            pre = units(0, half, m, sent[half])
            keep[0, half, slots(m), :] = pre
            put(act.at[0], half, m, jax.nn.silu(pre).astype(BF))
            done.append(sp1(act.at[0], half, m))
        return done

    own1, got1 = 1 + pipe, 1 + other
    for copy in own_load:
        copy.wait()
    e0 = {i: remote(own.at[pipe, cuts[i], :], w.at[3 * pipe, core, z, cuts[i], :], pair) for i in order}
    e1 = remote(own.at[other], w.at[own1, core, z], pair)
    x_load.wait()
    x_here, x_swap = swap_tokens(0, x0)
    ca_own1 = g1(own1, lo)
    cot_load.wait()
    cot_here, cot_swap = swap_tokens(1, cot)
    ca0 = {}
    for i in order:
        e0[i].wait_recv()
        ca0[i] = g1(0, cuts[i])
    cb0 = Group(w.at[0, core, z])
    for i in order:
        wait_all(ca0[i])
        ahead, to = (zd, up) if i < 2 else (zu, dn)
        ref = w.at[0, core, ahead, cuts[i], :]
        cb0.send(ref, ref, to)
    cc0 = g2c(0)
    ca3 = g1(3)
    ca_own1 += g1(own1, hi)
    e1.wait_recv()
    ca_got1 = g1(got1)
    cb0.wait_recv()
    cd0 = g3(0)
    x_here.wait()
    wait_all(x_swap)
    wait_all(cc0)
    wait_all(cd0)

    project(x0, 0, 0, 0, 0)
    p00a = rs1(0, 0, 0)
    project(x0, 0, 0, 1, 0)
    p00b = rs1_turned(0, 0)
    p01 = project_send(x0, 0, 0, 1)
    wait_all(ca3)
    cb3 = g2(3)
    cc3 = g2c(3)
    wait_all(ca_own1)
    cb_own1 = g2(own1)
    cc_own1 = g2c(own1)
    p00 = [rs2(0, 0, 0, p00a), rs2_turned(0, 0, p00b)]
    p01 = all_rs2(0, 1, p01)
    a00 = open_act(0, p00)
    wait_all(ca_got1)
    cb_got1 = g2(got1)
    cc_got1 = g2c(got1)
    a01 = open_act(1, p01)
    a00 = all_sp2(act.at[0], 0, a00)
    wait_all(cb3)
    cd3 = g3(3)
    a01 = all_sp2(act.at[0], 1, a01)
    cot_here.wait()
    wait_all(cot_swap)
    wait_all(cc3)
    wait_all(cd3)
    p20 = project_send(cot, 3, 2, 0)
    p21 = project_send(cot, 3, 2, 1)
    wait_all(cb_own1)
    cd_own1 = g3(own1)
    wait_all(cb_got1)
    cd_got1 = g3(got1)
    settle(a00)
    wait_all(cc_own1 + cc_got1)
    wait_all(cd_own1 + cd_got1)
    widen(x0, act.at[0], 1, x1, 0)
    p10 = project_send(x1, 2, 1, 0)
    settle(a01)
    widen(x0, act.at[0], 1, x1, 1)
    p11 = project_send(x1, 2, 1, 1)
    p20 = all_rs2(2, 0, p20)
    p21 = all_rs2(2, 1, p21)
    p10 = all_rs2(1, 0, p10)
    def open_slope(m, sent_up, sent_pre):
        done = []
        for half in HALVES:
            upward = units(2, half, m, sent_up[half])
            pre = units(1, half, m, sent_pre[half])
            put(slope.at[1], half, m, slope_of(upward, pre))
            done.append(sp1(slope.at[1], half, m))
            put(act.at[1], half, m, jax.nn.silu(pre).astype(BF))
        return done

    p11 = all_rs2(1, 1, p11)
    s10 = open_slope(0, p20, p10)
    s11 = open_slope(1, p21, p11)
    s10 = all_sp2(slope.at[1], 0, s10)
    s11 = all_sp2(slope.at[1], 1, s11)
    a10 = both(lambda half: sp1(act.at[1], half, 0))
    a11 = both(lambda half: sp1(act.at[1], half, 1))
    settle(s10)
    widen(cot, slope.at[1], 2, err1, 0)
    p30 = project_send(err1, 1, 3, 0)
    settle(s11)
    d2, near2 = weight_grad(x1, slope.at[1], 2)
    widen(cot, slope.at[1], 2, err1, 1)
    p31 = project_send(err1, 1, 3, 1)
    d2 = q1(2, d2)
    a10 = all_sp2(act.at[1], 0, a10)
    p30 = all_rs2(3, 0, p30)
    p31 = all_rs2(3, 1, p31)
    a11 = all_sp2(act.at[1], 1, a11)
    d1, near1 = weight_grad(err1, act.at[0], 1)
    d2 = q2(2, d2, near2)
    def close_slope(m, sent):
        done = []
        for half in HALVES:
            upward = units(3, half, m, sent[half])
            put(slope.at[0], half, m, slope_of(upward, keep[0, half, slots(m), :]))
            done.append(sp1(slope.at[0], half, m))
        return done

    s00 = close_slope(0, p30)
    d1 = q1(1, d1)
    s01 = close_slope(1, p31)
    settle(a10)
    settle(a11)
    d3, near3 = weight_grad(cot, act.at[1], 3)
    s00 = all_sp2(slope.at[0], 0, s00)
    s01 = all_sp2(slope.at[0], 1, s01)
    d3 = q1(3, d3)
    d1 = q2(1, d1, near1)
    squares = finish(2, d2)
    settle(s00)
    settle(s01)
    d0, near0 = weight_grad(x0, slope.at[0], 0)
    d0 = q1(0, d0)
    d3 = q2(3, d3, near3)
    squares = squares + finish(1, d1)
    d0 = q2(0, d0, near0)
    squares = squares + finish(3, d3)
    h1 = hand_over(1)
    turned[0] = fin[2 * pipe + 1].T
    writes = [local(turned.at[0], tot_out.at[:, keep_rows])]
    squares = squares + finish(0, d0)
    nsum[0] = squares
    c1 = group_of(n2.at[pl.ds(1, 15)], [(nsum.at[0], n2.at[code], dev) for code, dev in xz])
    h0 = hand_over(0)
    writes.append(local(fin.at[2 * pipe], tot_in.at[keep_rows, :]))
    wait_all(c1)
    total = nsum[0]
    for code in range(1, 16):
        total = total + n2[code]
    nsum[1] = total
    c2 = group_of(n1.at[pl.ds(1, 7)], [(nsum.at[1], n1.at[code], dev) for code, dev, _, _ in ycore])
    h1.wait_recv()
    turned[1] = prx[1].astype(F32).T
    writes.append(local(turned.at[1], tot_out.at[:, give_rows]))
    wait_all(c2)
    total = nsum[1]
    for code in range(1, 8):
        total = total + n1[code]
    norm = jnp.sqrt(jnp.sum(total, keepdims=True))
    norm_out[...] = norm
    h0.wait_recv()
    late[...] = prx[0].astype(F32)
    writes.append(local(late, tot_in.at[give_rows, :]))
    for copy in started:
        copy.wait_send()
    for copy in writes:
        copy.wait()


def clip(norm_ref, tot_in, tot_out, upd_in, upd_out):
    factor = jnp.minimum(1.0, CLIP_NORM / norm_ref[...])
    upd_in[...] = tot_in[...] * factor
    upd_out[...] = tot_out[...] * factor


def on_device(inputs, w_in, w_out, cotangent):
    micro, tok, cols = inputs.shape
    shard, hid = w_in.shape[1], w_in.shape[2]
    sub = shard // 2
    part_d = cols // 4
    group = micro * tok // 2
    hl = hid // 2
    any_spec = pl.BlockSpec(memory_space=pl.ANY)
    vmem = pl.BlockSpec(memory_space=pltpu.VMEM)
    tokens = pltpu.VMEM((RING, micro, tok // 2, part_d), BF)
    weights = pltpu.VMEM((4, 2, RING, sub, hid), BF)
    layers = pltpu.VMEM((2, RING, group, hid), BF)
    tot_in, tot_out, norm = pl.pallas_call(
        kernel,
        out_shape=(
            jax.ShapeDtypeStruct((shard, hid), F32),
            jax.ShapeDtypeStruct((hid, shard), F32),
            jax.ShapeDtypeStruct((1, 1), F32),
        ),
        in_specs=[any_spec] * 4,
        out_specs=(any_spec, any_spec, vmem),
        scratch_shapes=[
            pltpu.VMEM((2, RING, micro, tok, RING * sub), BF),
            tokens, tokens, tokens, tokens,
            pltpu.VMEM((2, hid, sub), BF),
            pltpu.VMEM((2, sub, hid), BF),
            weights, weights, layers, layers,
            pltpu.VMEM((4, RING, group, hid), BF),
            pltpu.VMEM((4, 2 * RING, group, hl), BF),
            pltpu.VMEM((RING, RING, group // 2 // RING, hl), BF),
            pltpu.VMEM((4, 2, RING, group // RING, hl), BF),
            pltpu.VMEM((2, 2, group // RING, hl), F32),
            pltpu.VMEM((4, RING, sub, hid), BF),
            pltpu.VMEM((4, 2, sub // 2, hid), BF),
            pltpu.VMEM((4, 2, sub, hid), BF),
            pltpu.VMEM((4, sub, hid), F32),
            pltpu.VMEM((2, sub, hid), BF),
            pltpu.VMEM((2, sub, hid), BF),
            pltpu.VMEM((sub, hid), F32),
            pltpu.VMEM((2, hid, sub), F32),
            pltpu.VMEM((2, 8, 128), F32),
            pltpu.VMEM((8, 8, 128), F32),
            pltpu.VMEM((16, 8, 128), F32),
            pltpu.SemaphoreType.DMA((12,)),
            pltpu.SemaphoreType.DMA((45,)),
            pltpu.SemaphoreType.DMA((111,)),
        ],
        compiler_params=pltpu.CompilerParams(
            collective_id=0, has_side_effects=True, vmem_limit_bytes=67043328
        ),
    )(inputs, w_in[0], w_out[0], cotangent)
    steps = 2
    in_block = pl.BlockSpec((shard // steps, hid), lambda i: (i, 0))
    out_block = pl.BlockSpec((hid // steps, shard), lambda i: (i, 0))
    upd_in, upd_out = pl.pallas_call(
        clip,
        grid=(steps,),
        out_shape=(jax.ShapeDtypeStruct((shard, hid), F32), jax.ShapeDtypeStruct((hid, shard), F32)),
        in_specs=[pl.BlockSpec((1, 1), lambda i: (0, 0)), in_block, out_block],
        out_specs=(in_block, out_block),
    )(norm, tot_in, tot_out)
    return upd_in[None], upd_out[None], norm[0, 0]


def solution(mesh):
    split = Mesh(mesh.devices.reshape(mesh.shape["pipe"], 2, 2, RING, RING), AXES)
    placed = (
        P(None, DP, TENSOR),
        P("pipe", TENSOR_DP, None),
        P("pipe", None, TENSOR_DP),
        P(None, DP, TENSOR),
    )
    return jax.shard_map(
        on_device,
        mesh=split,
        in_specs=placed,
        out_specs=(P("pipe", TENSOR_DP, None), P("pipe", None, TENSOR_DP), P()),
        check_vma=False,
    )
```
